32 devices in a mesh: gx: 4 (over y, core), gy: 8 (over z, x).
Axes of the slice: x: 2, y: 2, z: 4, core: 2. Of those that a mesh axis runs over, the one named last changes fastest.
Arguments:
- spectra: bfloat16 [4, 8, 3, 2, 128, 4096], P('gx', 'gy'), may hold values from -1000 to 1000
- partner_codes: int32 [4, 8, 5], P('gx', 'gy'), may hold values from -1 to 4, as said below
- range_bits: int32 [4, 8, 5, 128, 5], P('gx', 'gy'), may hold values from 0 to 1073741823
- old_stacks: float32 [4, 8, 5, 8, 2, 128, 128], P('gx', 'gy'), may hold values from -6 to 6
Outputs:
- stacks: float32 [4, 8, 5, 8, 2, 128, 128], P('gx', 'gy')
The draws below stay inside these ranges and needn't reach their ends.
Inputs may be any that keep to these rules, and one draw needn't show every extreme that they name: `partner_codes`: each block lists code 0 first, then further distinct codes in increasing order, then -1 in the remaining slots; no listed code names a block outside the grid of 4 x 8 blocks; some block lists all 5 codes.
All inputs are finite; a program needn't handle non-finite values.
Results may differ from the reference program's by a relative error of at most 0.0014.
Values may be sent and summed in bfloat16 or wider, within the bound.
A program may use at most 192 MiB of HBM per device.

```python
import math
import jax
import jax.numpy as jnp
from jax import lax

ST = 128
F = 4096
BANDS = 8
SLOTS = 5
SEG = 3
BW = 512
WORDS = 5
NBX = 4
NBY = 8


def draw_spectra(key, part):
    first_key = jax.random.fold_in(key, 11)
    second_key = jax.random.fold_in(key, 12)
    third_key = jax.random.fold_in(key, 13)
    full_shape = (NBX, NBY, SEG, 2, ST, F)
    base_noise = jax.random.truncated_normal(first_key, -6.0, 6.0, full_shape, jnp.float32)
    spread = math.log(10.0)
    bin_scale = jnp.exp(spread * jax.random.uniform(second_key, (NBX, NBY, SEG, 1, ST, F), jnp.float32))
    band_scale = jnp.exp(math.log(10.0) * jax.random.uniform(third_key, (NBX, NBY, 1, 1, ST, BANDS, 1), jnp.float32))
    band_full = jnp.broadcast_to(band_scale, (NBX, NBY, 1, 1, ST, BANDS, BW)).reshape(NBX, NBY, 1, 1, ST, F)
    return (base_noise * bin_scale * band_full).astype(jnp.bfloat16)


def draw_partner_codes(key, part):
    row_pos = jnp.arange(NBX, dtype=jnp.int32)[:, None]
    col_pos = jnp.arange(NBY, dtype=jnp.int32)[None, :]
    first_level = jax.random.randint(jax.random.fold_in(key, 21), (NBX, NBY), 0, 10, dtype=jnp.int32)
    second_level = jax.random.randint(jax.random.fold_in(key, 22), (NBX, NBY), 0, 10, dtype=jnp.int32)
    density = first_level * second_level + first_level + second_level + 1
    trials = jax.random.randint(jax.random.fold_in(key, 23), (NBX, NBY, 4), 0, 100, dtype=jnp.int32)
    forced_row = jax.random.randint(jax.random.fold_in(key, 24), (), 1, NBX - 1, dtype=jnp.int32)
    forced_col = jax.random.randint(jax.random.fold_in(key, 25), (), 0, NBY - 1, dtype=jnp.int32)
    forced = (row_pos == forced_row) & (col_pos == forced_col)
    step_rows = [1, -1, 0, 1]
    step_cols = [0, 1, 1, 1]
    listed = [jnp.ones((NBX, NBY), dtype=bool)]
    for which in range(4):
        target_row = row_pos + step_rows[which]
        target_col = col_pos + step_cols[which]
        inside = (target_row >= 0) & (target_row < NBX) & (target_col < NBY)
        listed.append(inside & ((trials[:, :, which] < density) | forced))
    valid = jnp.stack(listed, -1).astype(jnp.int32)
    ranks = jnp.cumsum(valid, -1) - 1
    counts = jnp.sum(valid, -1)
    code_values = jnp.arange(5, dtype=jnp.int32)
    slots_out = []
    for slot_index in range(SLOTS):
        matched = valid * (ranks == slot_index).astype(jnp.int32)
        chosen = jnp.sum(matched * code_values, -1)
        slots_out.append(jnp.where(counts > slot_index, chosen, -1).astype(jnp.int32))
    return jnp.stack(slots_out, -1)


def touch_ends(drawn, key, smallest, largest):
    spot = [jax.random.randint(jax.random.fold_in(key, axis), (), 0, length) for axis, length in enumerate(drawn.shape)]
    widest = drawn.shape.index(max(drawn.shape))
    neighbour = spot[:widest] + [(spot[widest] + 1) % drawn.shape[widest]] + spot[widest + 1:]
    return drawn.at[tuple(spot)].set(smallest).at[tuple(neighbour)].set(largest)


def shard_levels(rng, extent, pieces, smallest, top_value):
    loudness, own = 1.0, jax.random.fold_in(rng, 6)
    for axis_at, shards_of in pieces:
        heights = jnp.exp(jax.random.uniform(jax.random.fold_in(own, axis_at), (shards_of,), jnp.float32, smallest / len(pieces), top_value / len(pieces)))
        loudness = loudness * jnp.repeat(heights, extent[axis_at] // shards_of).reshape([-1 if axis == axis_at else 1 for axis in range(len(extent))])
    return loudness


def centred(own_key, dims, width, limit, cuts=(), kind=jnp.bfloat16):
    array = width * jax.random.normal(own_key, dims, jnp.float32)
    if cuts:
        array = array * shard_levels(own_key, dims, cuts, -0.22, 0.18)
    return jnp.clip(array, -limit, limit).astype(kind)


def setup_inputs(seed: int = 0) -> dict:
    keys = jax.random.split(jax.random.key(seed), 5)
    return {
        "spectra": draw_spectra(jax.random.fold_in(keys[4], 71), 0),
        "partner_codes": draw_partner_codes(jax.random.fold_in(keys[4], 71), 0),
        "range_bits": touch_ends(jax.random.randint(keys[2], (NBX, NBY, SLOTS, ST, WORDS), 0, 1073741824), jax.random.fold_in(keys[2], 1), 0, 1073741823).astype(jnp.int32),
        "old_stacks": centred(keys[3], (NBX, NBY, SLOTS, BANDS, 2, ST, ST), 1.0, 6.0, ((0, 4), (1, 8)), jnp.float32),
    }


EPSILON = 1e-06

def whiten(spectrum, band_count):
    segments, components, stations, freq_bins = spectrum.shape
    grouped = spectrum.astype(jnp.float32).reshape(segments, components, stations, band_count, freq_bins // band_count)
    band_power = lax.optimization_barrier(jnp.mean(grouped * grouped, axis=(0, 1, 4)))
    scaled = grouped * lax.rsqrt(band_power + EPSILON)[None, None, :, :, None]
    return scaled.reshape(spectrum.shape).astype(jnp.bfloat16)

def cross_bands(first_block, second_block, band_count):
    segments, components, stations, freq_bins = first_block.shape
    band_width = freq_bins // band_count
    first_wide = first_block.astype(jnp.float32)
    turned = jnp.stack([first_wide[:, 1], -first_wide[:, 0]], axis=1)
    stacked = jnp.stack([first_wide, turned], 0).reshape(2, segments, components, stations, band_count, band_width)
    partner_wide = second_block.astype(jnp.float32).reshape(segments, components, stations, band_count, band_width)
    product = jnp.einsum('oscinw,scjnw->noij', stacked, partner_wide, precision=lax.Precision.HIGHEST)
    return product * (1.0 / math.sqrt(segments * band_width))

def unpack_range(range_words, stations):
    word_count = range_words.shape[-1]
    column_ids = jnp.arange(stations, dtype=jnp.int32)
    onehot = (column_ids[:, None] // 30 == jnp.arange(word_count, dtype=jnp.int32)[None, :]).astype(jnp.int32)
    selected = lax.optimization_barrier(jnp.sum(range_words[..., :, None, :] * onehot, axis=-1))
    flags = jnp.bitwise_and(jnp.right_shift(selected, column_ids % 30), 1)
    return flags.astype(jnp.float32)

def reference(spectra, partner_codes, range_bits, old_stacks):
    row_count = spectra.shape[0]
    col_count = spectra.shape[1]
    block_count = row_count * col_count
    band_count = old_stacks.shape[3]
    stations = old_stacks.shape[-1]
    slot_count = partner_codes.shape[-1]
    flat_spectra = spectra.reshape((block_count,) + spectra.shape[2:])
    whitened = lax.map(lambda spectrum: whiten(spectrum, band_count), flat_spectra).reshape(spectra.shape)

    def per_block(item):
        block_index, code_row, range_words, old_block = item
        row_pos = block_index // col_count
        col_pos = block_index % col_count
        own_block = whitened[row_pos, col_pos]
        unit_zero = jnp.zeros((band_count, 2, stations, stations), jnp.float32)
        crosses = []
        for slot_index in range(slot_count):
            pair_code = code_row[slot_index]
            step_row = (pair_code == 1).astype(jnp.int32) + (pair_code == 4).astype(jnp.int32) - (pair_code == 2).astype(jnp.int32)
            step_col = (pair_code >= 2).astype(jnp.int32)
            target_row = jnp.clip(row_pos + step_row, 0, row_count - 1)
            target_col = jnp.clip(col_pos + step_col, 0, col_count - 1)
            partner_block = whitened[target_row, target_col]
            pair_cross = lax.cond(pair_code >= 0, lambda operands: cross_bands(operands[0], operands[1], band_count).astype(jnp.float32), lambda operands: unit_zero, (own_block, partner_block))
            crosses.append(pair_cross)
        cross_all = jnp.stack(crosses, 0)
        in_range = unpack_range(range_words, stations)
        return old_block + in_range[:, None, None] * cross_all
    flat_items = (jnp.arange(block_count, dtype=jnp.int32), partner_codes.reshape(block_count, slot_count), range_bits.reshape((block_count,) + range_bits.shape[2:]), old_stacks.reshape((block_count,) + old_stacks.shape[2:]))
    updated = lax.map(per_block, flat_items)
    return updated.reshape(old_stacks.shape)
```

```python
import functools
import math

import jax
import jax.numpy as jnp
from jax import lax
from jax.experimental import pallas as pl
from jax.experimental.pallas import tpu as pltpu
from jax.sharding import PartitionSpec as P

EPSILON = 1e-06
MESH = pl.DeviceIdType.MESH
FLAG_BITS = 30


def whiten_block(ref, index):
    segments, parts, stations, width = ref.shape[len(index):]
    chunk = 16

    def rows(i, _):
        at = pl.ds(pl.multiple_of(i * chunk, chunk), chunk)
        pieces = [ref[(*index, s, p, at)].astype(jnp.float32)
                  for s in range(segments) for p in range(parts)]
        total = pieces[0] * pieces[0]
        for v in pieces[1:]:
            total = total + v * v
        power = jnp.sum(total, axis=1, keepdims=True) * (1.0 / (len(pieces) * width))
        scale = lax.rsqrt(power + EPSILON)
        for s in range(segments):
            for p in range(parts):
                ref[(*index, s, p, at)] = (pieces[s * parts + p] * scale).astype(jnp.bfloat16)
        return 0

    lax.fori_loop(0, stations // chunk, rows, 0, unroll=2)


def product(left, right, scale):
    segments = left.count
    total = None
    for s in range(segments):
        part = lax.dot_general(
            left(s), right(s), (((1,), (1,)), ((), ())), preferred_element_type=jnp.float32
        )
        total = part if total is None else total + part
    n = total.shape[0] // 2
    real = total[:n, :n] + total[n:, n:]
    imag = total[n:, :n] - total[:n, n:]
    return real * scale, imag * scale


class View:
    def __init__(self, ref, index, count):
        self.ref, self.index, self.count = ref, index, count

    def __call__(self, s):
        v = self.ref[(*self.index, s)]
        return v.reshape(v.shape[0] * v.shape[1], v.shape[2])


OTHER = 3


def cross_kernel(rows, cols, x_ref, self_ref, c_ref, blk, stage,
                 load_sem, xs, xr, zs, zr, ys, yr, rs, rr):
    half, segments, width = blk.shape[1], blk.shape[3], blk.shape[6]
    scale = 1.0 / math.sqrt(segments * width)
    r = lax.axis_index("gx")
    c = lax.axis_index("gy")
    odd = lax.rem(c, 2)
    mate = c + 1 - 2 * odd
    keep_slot = 2 * odd
    halo_slot = 2 - 2 * odd
    z_to = c - 2 + 4 * odd
    z_from = c + 2 - 4 * odd
    sends_z = (z_to >= 0) & (z_to < cols)
    has_halo = (z_from >= 0) & (z_from < cols)
    first_col = c - 2 * odd

    def load(b, mine):
        band = half * (odd if mine else 1 - odd) + b
        at = pl.ds(pl.multiple_of(band * width, width), width)
        slot = keep_slot if mine else OTHER
        return pltpu.make_async_copy(
            x_ref.at[0, 0, :, :, :, at], blk.at[0, b, slot], load_sem.at[int(mine), b])

    def x_copy(b, s):
        return pltpu.make_async_remote_copy(
            src_ref=blk.at[0, b, OTHER, s], dst_ref=blk.at[0, b, 1, s],
            send_sem=xs.at[0], recv_sem=xr.at[b, s],
            device_id=(r, mate), device_id_type=MESH)

    def z_copy(b, s):
        return pltpu.make_async_remote_copy(
            src_ref=blk.at[0, b, keep_slot, s], dst_ref=blk.at[0, b, halo_slot, s],
            send_sem=zs.at[0], recv_sem=zr.at[b, s], device_id=(r, z_to), device_id_type=MESH)

    def y_row(b):
        return r - 1 + 2 * lax.rem(b, 2)

    def y_sends(b):
        to = y_row(b)
        return (to >= 0) & (to < rows)

    def y_meets(b):
        other_row = r + 1 - 2 * lax.rem(b, 2)
        return (other_row >= 0) & (other_row < rows)

    def y_copy(b, slot, s, group=0):
        return pltpu.make_async_remote_copy(
            src_ref=blk.at[0, b, slot, s], dst_ref=blk.at[1, b, slot, s],
            send_sem=ys.at[b], recv_sem=yr.at[b, group],
            device_id=(y_row(b), c), device_id_type=MESH)

    def y_taken(b, slots, group):
        return pltpu.make_async_remote_copy(
            src_ref=blk.at[0, b, pl.ds(0, slots)], dst_ref=blk.at[1, b, pl.ds(0, slots)],
            send_sem=ys.at[b], recv_sem=yr.at[b, group],
            device_id=(y_row(b), c), device_id_type=MESH)

    def r_copy(b, which, code, band, row, col):
        group = {1: 0, 0: 1, 2: 2, 3: 2, 5: 3, 7: 3, 4: 5, 6: 7}[which]
        return pltpu.make_async_remote_copy(
            src_ref=stage.at[b, which], dst_ref=c_ref.at[code - 1, band],
            send_sem=rs.at[group + lax.rem(b, 2) if group > 2 else group], recv_sem=rr.at[code - 1],
            device_id=(row, col), device_id_type=MESH)

    def r_whole(group, code, count):
        return pltpu.make_async_remote_copy(
            src_ref=c_ref.at[0, pl.ds(0, count)], dst_ref=c_ref.at[0, pl.ds(0, count)],
            send_sem=rs.at[group], recv_sem=rr.at[code - 1],
            device_id=(r, mate), device_id_type=MESH)

    def load_band(b, _):
        pl.when(b > 0)(load(b, False).start)
        load(b, True).start()
        return 0

    def send_band(b, _):
        @pl.when(b > 0)
        def _():
            load(b, False).wait()
            whiten_block(blk, (0, b, OTHER))

        for s in range(segments):
            x_copy(b, s).start()
        load(b, True).wait()
        whiten_block(blk, (0, b, keep_slot))

        @pl.when(sends_z)
        def _():
            for s in range(segments):
                z_copy(b, s).start()

        @pl.when(y_sends(b))
        def _():
            for slot in (keep_slot, OTHER):
                for s in range(segments):
                    y_copy(b, slot, s).start()
        return 0

    load(0, False).start()
    barrier = pltpu.get_barrier_semaphore()
    peers = jnp.int32(0)
    for dr in (-1, 0, 1):
        for col in (mate, c - 2, c + 2) if dr == 0 else (c, mate, c - 2, c + 2):
            there = (r + dr >= 0) & (r + dr < rows) & (col >= 0) & (col < cols)
            peers = peers + there.astype(jnp.int32)

            @pl.when(there)
            def _():
                pl.semaphore_signal(barrier, inc=1, device_id=(r + dr, col), device_id_type=MESH)
    load(0, False).wait()
    lax.fori_loop(0, half, load_band, 0)
    whiten_block(blk, (0, 0, OTHER))
    pl.semaphore_wait(barrier, peers)
    lax.fori_loop(0, half, send_band, 0)

    def own_product(b, _):
        for slot, band in ((keep_slot, half * odd + b), (OTHER, half * (1 - odd) + b)):
            view = View(blk, (0, b, slot), segments)
            real, imag = product(view, view, scale)
            self_ref[band, 0] = real
            self_ref[band, 1] = imag
        return 0

    left_pair = (odd == 0) | has_halo
    right_pair = (odd == 1) | has_halo

    def routes(b):
        is_odd = lax.rem(b, 2)
        meets = y_meets(b)
        top = r - is_odd
        t, m = is_odd, 1 - is_odd
        band, other_band = half * odd + b, half * (1 - odd) + b
        return [
            (0, (0, 0), (0, 1), 3, band, r, first_col, left_pair, odd == 0),
            (1, (0, 1), (0, 2), 3, band, r, mate, right_pair, None),
            (2, (t, keep_slot), (m, keep_slot), 1, band, top, c, meets, is_odd == 0),
            (3, (t, OTHER), (m, OTHER), 1, other_band, top, c, meets, is_odd == 0),
            (4, (t, 0), (m, 1), 4, band, top, first_col, meets & left_pair, (odd == 0) & (is_odd == 0)),
            (5, (t, 1), (m, 2), 4, band, top, mate, meets & right_pair, None),
            (6, (m, 0), (t, 1), 2, band, top + 1, first_col, meets & left_pair, (odd == 0) & (is_odd == 1)),
            (7, (m, 1), (t, 2), 2, band, top + 1, mate, meets & right_pair, None),
        ]

    def emit(b, route, go=True):
        which, left, right, code, band, row, col, present, local = route

        @pl.when(present)
        def _():
            real, imag = product(View(blk, (left[0], b, left[1]), segments),
                                 View(blk, (right[0], b, right[1]), segments), scale)
            real, imag = real.astype(jnp.bfloat16), imag.astype(jnp.bfloat16)

            def remote():
                stage[b, which, 0] = real
                stage[b, which, 1] = imag
                pl.when(go)(r_copy(b, which, code, band, row, col).start)

            if local is None:
                remote()
            else:
                @pl.when(local)
                def _():
                    c_ref[code - 1, band, 0] = real
                    c_ref[code - 1, band, 1] = imag

                pl.when(jnp.logical_not(local))(remote)

    def step(b, _):
        @pl.when(b < half)
        def _():
            for s in range(segments):
                x_copy(b, s).wait_recv()

                @pl.when(y_sends(b))
                def _():
                    y_copy(b, 1, s, 1).start()

                @pl.when(has_halo)
                def _():
                    z_copy(b, s).wait_recv()

                    @pl.when(y_sends(b))
                    def _():
                        y_copy(b, halo_slot, s, 2).start()

            @pl.when(b == half - 1)
            def _():
                for a in range(half - 1):
                    table = routes(a)
                    for which in (1, 5, 7) if a < half - 2 else (1,):
                        _, _, _, code, band, row, col, present, _ = table[which]
                        pl.when(present)(r_copy(a, which, code, band, row, col).start)

            @pl.when(y_meets(b))
            def _():
                y_taken(b, 2, 0).wait_recv()

            table = routes(b)
            for which in (1, 0, 2, 3):
                emit(b, table[which], b == half - 1 if which == 1 else True)

        @pl.when(b > 0)
        def _():
            a = b - 1

            @pl.when(y_meets(a))
            def _():
                y_taken(a, 1, 1).wait_recv()

                @pl.when(has_halo)
                def _():
                    y_taken(a, 1, 2).wait_recv()

            table = routes(a)
            for which in (5, 7, 4, 6):
                emit(a, table[which], a >= half - 2 if which in (5, 7) else True)
        return 0

    lax.fori_loop(0, half, own_product, 0)
    lax.fori_loop(0, half + 1, step, 0)

    def sent(slots, index, sem):
        return pltpu.make_async_remote_copy(
            src_ref=slots, dst_ref=slots, send_sem=sem.at[index], recv_sem=xr.at[0, 0],
            device_id=(r, mate), device_id_type=MESH)

    sent(blk.at[0, :, OTHER], 0, xs).wait_send()

    @pl.when(sends_z)
    def _():
        sent(blk.at[0, :, OTHER], 0, zs).wait_send()

    def finish(b, _):
        @pl.when(y_sends(b) & has_halo)
        def _():
            sent(blk.at[0, b], b, ys).wait_send()

        @pl.when(y_sends(b) & jnp.logical_not(has_halo))
        def _():
            sent(blk.at[0, b, pl.ds(0, 3)], b, ys).wait_send()
        return 0

    lax.fori_loop(0, half, finish, 0)

    turns = [(half + 1 - parity) // 2 for parity in (0, 1)]
    pl.when(right_pair)(r_whole(0, 1, half).wait_send)
    pl.when(left_pair & (odd == 1))(r_whole(1, 1, half).wait_send)
    pl.when(y_meets(1))(r_whole(2, 1, 2 * turns[1]).wait_send)
    for parity in (0, 1):
        meets = y_meets(parity)
        pl.when(meets & right_pair)(r_whole(3 + parity, 1, 2 * turns[parity]).wait_send)
        for group, near in ((5, parity == 0), (7, parity == 1)):
            gone = meets & left_pair & ((odd == 1) if near else True)
            pl.when(gone)(r_whole(group + parity, 1, turns[parity]).wait_send)

    next_col = c + 1 < cols
    below = r + 1 < rows
    above = r > 0
    pl.when(below)(r_whole(0, 1, 2 * turns[1]).wait_recv)
    for code, comes, near in ((2, above & next_col, turns[1]), (3, next_col, half),
                              (4, below & next_col, turns[0])):
        pl.when(comes & (odd == 1))(r_whole(0, code, 2 * half).wait_recv)
        pl.when(comes & (odd == 0))(r_whole(0, code, 2 * half - near).wait_recv)


def crosses(spectra, bands, rows, cols):
    segments, parts, stations, bins = spectra.shape[2:]
    half, width = bands // 2, bins // bands
    dma = pltpu.SemaphoreType.DMA
    return pl.pallas_call(
        functools.partial(cross_kernel, rows, cols),
        out_shape=(
            jax.ShapeDtypeStruct((bands, 2, stations, stations), jnp.float32),
            jax.ShapeDtypeStruct((4, bands, 2, stations, stations), jnp.bfloat16),
        ),
        in_specs=[pl.BlockSpec(memory_space=pltpu.MemorySpace.HBM)],
        out_specs=(pl.BlockSpec(memory_space=pltpu.VMEM), pl.BlockSpec(memory_space=pltpu.VMEM)),
        scratch_shapes=[
            pltpu.VMEM((2, half, 4, segments, parts, stations, width), jnp.bfloat16),
            pltpu.VMEM((half, 8, 2, stations, stations), jnp.bfloat16),
            dma((2, half)),
            dma((1,)), dma((half, segments)),
            dma((1,)), dma((half, segments)),
            dma((half,)), dma((half, 3)),
            dma((9,)), dma((4,)),
        ],
        compiler_params=pltpu.CompilerParams(collective_id=0, has_side_effects=True, vmem_limit_bytes=48 * 1024 * 1024),
        name="crosses",
    )(spectra)


def combine_kernel(codes, self_ref, c_ref, bits_ref, old_ref, out_ref, done, sem):
    slots, bands = old_ref.shape[2:4]
    words, stations = bits_ref.shape[2], bits_ref.shape[4]
    column = lax.broadcasted_iota(jnp.int32, (stations, stations), 0)

    def write(s):
        return pltpu.make_async_copy(done.at[s], out_ref.at[0, 0, s], sem.at[s])

    for s in range(slots):
        code = codes[s]
        chosen = jnp.zeros((stations, stations), jnp.int32)
        bit = column
        for w in range(words):
            reached = column >= w * FLAG_BITS
            chosen = jnp.where(reached, bits_ref[0, s, w], chosen)
            bit = jnp.where(reached, column - w * FLAG_BITS, bit)
        flags = jnp.bitwise_and(jnp.right_shift(chosen, bit), 1).astype(jnp.float32).T > 0.5

        @pl.when(code == 0)
        def _():
            for k in range(bands):
                done[s, k] = old_ref[0, 0, s, k] + jnp.where(flags, self_ref[k], 0.0)

        @pl.when(code > 0)
        def _():
            for k in range(bands):
                done[s, k] = old_ref[0, 0, s, k] + jnp.where(
                    flags, c_ref[code - 1, k].astype(jnp.float32), 0.0)

        @pl.when(code < 0)
        def _():
            done[s] = old_ref[0, 0, s]

        write(s).start()
    for s in range(slots):
        write(s).wait()


def combine(codes, own, cross, range_bits, old):
    slots, bands, parts, stations = old.shape[2:6]
    vmem = pl.BlockSpec(memory_space=pltpu.VMEM)
    return pl.pallas_call(
        combine_kernel,
        out_shape=jax.ShapeDtypeStruct(old.shape, old.dtype),
        in_specs=[pl.BlockSpec(memory_space=pltpu.SMEM), vmem, vmem, vmem, vmem],
        out_specs=pl.BlockSpec(memory_space=pltpu.MemorySpace.HBM),
        scratch_shapes=[
            pltpu.VMEM((slots, bands, parts, stations, stations), jnp.float32),
            pltpu.SemaphoreType.DMA((slots,)),
        ],
        compiler_params=pltpu.CompilerParams(vmem_limit_bytes=20 * 1024 * 1024),
        name="combine",
    )(codes, own, cross, jnp.transpose(range_bits, (0, 2, 4, 1, 3)), old)


def solution(mesh):
    rows, cols = mesh.shape["gx"], mesh.shape["gy"]

    def body(spectra, partner_codes, range_bits, old_stacks):
        own, cross = crosses(spectra, old_stacks.shape[3], rows, cols)
        return combine(partner_codes[0, 0], own, cross, range_bits, old_stacks)

    return jax.shard_map(
        body,
        mesh=mesh,
        in_specs=(
            P("gx", "gy", None, None, None, None),
            P("gx", "gy", None),
            P("gx", "gy", None, None, None),
            P("gx", "gy", None, None, None, None, None),
        ),
        out_specs=P("gx", "gy", None, None, None, None, None),
        check_vma=False,
    )
```

```python
import functools
import math

import jax
import jax.numpy as jnp
from jax import lax
from jax.experimental import pallas as pl
from jax.experimental.pallas import tpu as pltpu
from jax.sharding import PartitionSpec as P

EPSILON = 1e-06
MESH = pl.DeviceIdType.MESH
FLAG_BITS = 30


def whiten_rows(ref, index, first, count):
    segments, parts, _, width = ref.shape[len(index):]
    chunk = 16

    def rows(i, _):
        at = pl.ds(pl.multiple_of(first + i * chunk, chunk), chunk)
        pieces = [ref[(*index, s, p, at)].astype(jnp.float32)
                  for s in range(segments) for p in range(parts)]
        total = pieces[0] * pieces[0]
        for v in pieces[1:]:
            total = total + v * v
        power = jnp.sum(total, axis=1, keepdims=True) * (1.0 / (len(pieces) * width))
        scale = lax.rsqrt(power + EPSILON)
        for s in range(segments):
            for p in range(parts):
                ref[(*index, s, p, at)] = (pieces[s * parts + p] * scale).astype(jnp.bfloat16)
        return 0

    lax.fori_loop(0, count // chunk, rows, 0, unroll=2)


def product(left, right, scale):
    segments = left.count
    total = None
    for s in range(segments):
        part = lax.dot_general(
            left(s), right(s), (((1,), (1,)), ((), ())), preferred_element_type=jnp.float32
        )
        total = part if total is None else total + part
    n = total.shape[0] // 2
    real = total[:n, :n] + total[n:, n:]
    imag = total[n:, :n] - total[:n, n:]
    return real * scale, imag * scale


class View:
    def __init__(self, ref, index, count):
        self.ref, self.index, self.count = ref, index, count

    def __call__(self, s):
        v = self.ref[(*self.index, s)]
        return v.reshape(v.shape[0] * v.shape[1], v.shape[2])


OTHER = 3
PIECES = 4
AHEAD = 4
ACROSS = (1, 5, 7)
ORDER = (1, 5, 7, 0, 4, 6, 2, 3)
GROUP = (3, 0, 6, 6, 4, 1, 5, 2)


def cross_kernel(rows, cols, x_ref, self_ref, c_ref, both, stage,
                 first_sem, load_sem, xs, xr, zs, zr, ms, mr, ks, kr, rs, rr):
    blk, far = both.at[0], both.at[1]
    half, segments, stations, width = both.shape[1], both.shape[3], both.shape[5], both.shape[6]
    scale = 1.0 / math.sqrt(segments * width)
    piece = stations // PIECES
    turns = [(half + 1 - parity) // 2 for parity in (0, 1)]
    r = lax.axis_index("gx")
    c = lax.axis_index("gy")
    odd = lax.rem(c, 2)
    mate = c + 1 - 2 * odd
    keep_slot = 2 * odd
    halo_slot = 2 - 2 * odd
    z_to = c - 2 + 4 * odd
    z_from = c + 2 - 4 * odd
    sends_z = (z_to >= 0) & (z_to < cols)
    has_halo = (z_from >= 0) & (z_from < cols)
    first_col = c - 2 * odd
    above = r > 0
    below = r + 1 < rows
    left_pair = (odd == 0) | has_halo
    right_pair = (odd == 1) | has_halo

    def strip(q):
        return pl.ds(q * piece if isinstance(q, int) else pl.multiple_of(q * piece, piece), piece)

    def bins(b, mine):
        band = half * (odd if mine else 1 - odd) + b
        return pl.ds(pl.multiple_of(band * width, width), width)

    def load(b, mine):
        slot = keep_slot if mine else OTHER
        return pltpu.make_async_copy(
            x_ref.at[0, 0, :, :, :, bins(b, mine)], blk.at[b, slot], load_sem.at[int(mine), b])

    def load_first(q):
        return pltpu.make_async_copy(
            x_ref.at[0, 0, :, :, strip(q), bins(0, False)], blk.at[0, OTHER, :, :, strip(q)],
            first_sem.at[q])

    def x_copy(b, q):
        return pltpu.make_async_remote_copy(
            src_ref=blk.at[b, OTHER, :, :, strip(q)], dst_ref=blk.at[b, 1, :, :, strip(q)],
            send_sem=xs.at[0], recv_sem=xr.at[b, q],
            device_id=(r, mate), device_id_type=MESH)

    def z_copy(b):
        return pltpu.make_async_remote_copy(
            src_ref=blk.at[b, keep_slot], dst_ref=blk.at[b, halo_slot],
            send_sem=zs.at[0], recv_sem=zr.at[b], device_id=(r, z_to), device_id_type=MESH)

    def mid_copy(b, q, d):
        return pltpu.make_async_remote_copy(
            src_ref=blk.at[b, 1, :, :, strip(q)], dst_ref=far.at[b, d, :, :, strip(q)],
            send_sem=ms.at[d], recv_sem=mr.at[b, d],
            device_id=(r + 1 - 2 * d, c), device_id_type=MESH)

    def side_to(parity):
        return r - 1 + 2 * parity

    def sides(parity):
        to = side_to(parity)
        return (to >= 0) & (to < rows)

    def meets(parity):
        other_row = r + 1 - 2 * parity
        return (other_row >= 0) & (other_row < rows)

    def side_copy(parity, step):
        b = 2 * (step // (2 * PIECES)) + parity
        e = lax.rem(step // PIECES, 2)
        q = lax.rem(step, PIECES)
        slot = keep_slot + e * (OTHER - keep_slot)
        return pltpu.make_async_remote_copy(
            src_ref=blk.at[b, slot, :, :, strip(q)], dst_ref=far.at[b, 2 + e, :, :, strip(q)],
            send_sem=ks.at[parity], recv_sem=kr.at[b],
            device_id=(side_to(parity), c), device_id_type=MESH)

    def whole(slots, send, recv):
        return pltpu.make_async_remote_copy(
            src_ref=slots, dst_ref=slots, send_sem=send, recv_sem=recv,
            device_id=(r, mate), device_id_type=MESH)

    def r_copy(b, which, code, band, row, col):
        return pltpu.make_async_remote_copy(
            src_ref=stage.at[b, which], dst_ref=c_ref.at[code - 1, band],
            send_sem=rs.at[GROUP[which]], recv_sem=rr.at[code - 1],
            device_id=(row, col), device_id_type=MESH)

    def results(count, send=0, code=1):
        return whole(c_ref.at[0, pl.ds(0, count)], rs.at[send], rr.at[code - 1])

    def load_band(b, _):
        pl.when(b > 0)(load(b, False).start)
        load(b, True).start()
        return 0

    def send_other(b):
        load(b, False).wait()
        whiten_rows(both, (0, b, OTHER), 0, stations)
        for q in range(PIECES):
            x_copy(b, q).start()

    def send_mine(b, _):
        load(b, True).wait()
        whiten_rows(both, (0, b, keep_slot), 0, stations)
        pl.when(sends_z)(z_copy(b).start)
        return 0

    for q in range(PIECES):
        load_first(q).start()
    barrier = pltpu.get_barrier_semaphore()
    peers = jnp.int32(0)
    for dr in (0, 1, -1):
        for col in (mate, c - 2, c + 2) if dr == 0 else (c, mate):
            there = (r + dr >= 0) & (r + dr < rows) & (col >= 0) & (col < cols)
            peers = peers + there.astype(jnp.int32)

            @pl.when(there)
            def _():
                pl.semaphore_signal(barrier, inc=1, device_id=(r + dr, col), device_id_type=MESH)
    lax.fori_loop(0, half, load_band, 0)
    for q in range(PIECES):
        load_first(q).wait()
        whiten_rows(both, (0, 0, OTHER), q * piece, piece)
        if q == 0:
            pl.semaphore_wait(barrier, peers)
        x_copy(0, q).start()
    lax.fori_loop(0, 2, send_mine, 0)
    for step in range(AHEAD):
        for parity in (0, 1):
            pl.when(sides(parity))(side_copy(parity, jnp.int32(step)).start)

    def send_rest(b, _):
        send_other(b)

        @pl.when(b > 1)
        def _():
            send_mine(b, 0)
        return 0

    lax.fori_loop(1, half, send_rest, 0)

    def own_product(b):
        for slot, band in ((keep_slot, half * odd + b), (OTHER, half * (1 - odd) + b)):
            view = View(both, (0, b, slot), segments)
            real, imag = product(view, view, scale)
            self_ref[band, 0] = real
            self_ref[band, 1] = imag

    def routes(b):
        is_odd = lax.rem(b, 2)
        even = is_odd == 0
        band, other_band = half * odd + b, half * (1 - odd) + b
        near = odd == 0
        left, mid, right = (0, b, 0), (0, b, 1), (0, b, 2)
        mid_above, mid_below = (1, b, 0), (1, b, 1)
        keeps = (is_odd, b, keep_slot + is_odd * (2 - keep_slot)), (1 - is_odd, b, 2 + is_odd * (keep_slot - 2))
        return [
            (0, left, mid, 3, band, r, first_col, left_pair, near),
            (1, mid, right, 3, band, r, mate, right_pair, None),
            (2, *keeps, 1, band, r - is_odd, c, meets(is_odd), even),
            (3, (is_odd, b, OTHER), (1 - is_odd, b, OTHER), 1, other_band, r - is_odd, c, meets(is_odd), even),
            (4, left, mid_below, 4, band, r, first_col, below & left_pair, near),
            (5, mid_above, right, 4, band, r - 1, mate, above & right_pair, None),
            (6, left, mid_above, 2, band, r, first_col, above & left_pair, near),
            (7, mid_below, right, 2, band, r + 1, mate, below & right_pair, None),
        ]

    def emit(b, route, go=True):
        which, left, right, code, band, row, col, present, local = route

        @pl.when(present)
        def _():
            real, imag = product(View(both, left, segments), View(both, right, segments), scale)
            real, imag = real.astype(jnp.bfloat16), imag.astype(jnp.bfloat16)

            def remote():
                stage[b, which, 0] = real
                stage[b, which, 1] = imag
                pl.when(go)(r_copy(b, which, code, band, row, col).start)

            if local is None:
                remote()
            else:
                @pl.when(local)
                def _():
                    c_ref[code - 1, band, 0] = real
                    c_ref[code - 1, band, 1] = imag

                pl.when(jnp.logical_not(local))(remote)

    def fire(a):
        table = routes(a)
        for which in ACROSS:
            _, _, _, code, band, row, col, present, _ = table[which]
            pl.when(present)(r_copy(a, which, code, band, row, col).start)

    def step(b, _):
        for q in range(PIECES):
            @pl.when(b < half)
            def _():
                if q == 3:
                    @pl.when(b == half - 1)
                    def _():
                        for a in range(half - 1):
                            fire(a)
                x_copy(b, q).wait_recv()
                for d, there in ((0, below), (1, above)):
                    pl.when(there)(mid_copy(b, q, d).start)
                at = b * PIECES + q + AHEAD
                for parity in (0, 1):
                    pl.when(sides(parity) & (at < 2 * PIECES * turns[parity]))(side_copy(parity, at).start)

            @pl.when(b == 0)
            def _():
                for a in range(q, half, PIECES):
                    own_product(a)

            @pl.when(b > 0)
            def _():
                a = b - 1
                table = routes(a)
                for which in ORDER[2 * q: 2 * q + 2]:
                    if which == 1:
                        pl.when(has_halo)(z_copy(a).wait_recv)
                    if which == 5:
                        pl.when(above)(whole(far.at[a, 0], ms.at[0], mr.at[a, 0]).wait_recv)
                    if which == 7:
                        pl.when(below)(whole(far.at[a, 1], ms.at[0], mr.at[a, 1]).wait_recv)
                    if which == 2:
                        pl.when(meets(lax.rem(a, 2)))(
                            whole(far.at[a, pl.ds(2, 2)], ks.at[0], kr.at[a]).wait_recv)
                    emit(a, table[which], a == half - 1 if which in ACROSS else True)
        return 0

    lax.fori_loop(0, half + 1, step, 0)

    whole(blk.at[:, OTHER], xs.at[0], xr.at[0, 0]).wait_send()
    pl.when(sends_z)(whole(blk.at[:, OTHER], zs.at[0], xr.at[0, 0]).wait_send)
    for d, there in ((0, below), (1, above)):
        pl.when(there)(whole(blk.at[:, 1], ms.at[d], xr.at[0, 0]).wait_send)
    for parity in (0, 1):
        pl.when(sides(parity))(
            whole(far.at[pl.ds(0, turns[parity]), pl.ds(2, 2)], ks.at[parity], xr.at[0, 0]).wait_send)
    for group, there in enumerate((right_pair, above & right_pair, below & right_pair)):
        pl.when(there)(results(half, group).wait_send)
    for group, there in enumerate((left_pair, below & left_pair, above & left_pair), 3):
        pl.when(there & (odd == 1))(results(half, group).wait_send)
    pl.when(meets(1))(results(2 * turns[1], 6).wait_send)

    next_col = c + 1 < cols
    pl.when(below)(results(2 * turns[1], code=1).wait_recv)
    for code, comes in ((2, above & next_col), (3, next_col), (4, below & next_col)):
        pl.when(comes & (odd == 1))(results(2 * half, code=code).wait_recv)
        pl.when(comes & (odd == 0))(results(half, code=code).wait_recv)


def crosses(spectra, bands, rows, cols):
    segments, parts, stations, bins = spectra.shape[2:]
    half, width = bands // 2, bins // bands
    dma = pltpu.SemaphoreType.DMA
    return pl.pallas_call(
        functools.partial(cross_kernel, rows, cols),
        out_shape=(
            jax.ShapeDtypeStruct((bands, 2, stations, stations), jnp.float32),
            jax.ShapeDtypeStruct((4, bands, 2, stations, stations), jnp.bfloat16),
        ),
        in_specs=[pl.BlockSpec(memory_space=pltpu.MemorySpace.HBM)],
        out_specs=(pl.BlockSpec(memory_space=pltpu.VMEM), pl.BlockSpec(memory_space=pltpu.VMEM)),
        scratch_shapes=[
            pltpu.VMEM((2, half, 4, segments, parts, stations, width), jnp.bfloat16),
            pltpu.VMEM((half, 8, 2, stations, stations), jnp.bfloat16),
            dma((PIECES,)), dma((2, half)),
            dma((1,)), dma((half, PIECES)),
            dma((1,)), dma((half,)),
            dma((2,)), dma((half, 2)),
            dma((2,)), dma((half,)),
            dma((7,)), dma((4,)),
        ],
        compiler_params=pltpu.CompilerParams(collective_id=0, has_side_effects=True, vmem_limit_bytes=48 * 1024 * 1024),
        name="crosses",
    )(spectra)


def combine_kernel(codes, self_ref, c_ref, bits_ref, old_ref, out_ref, done, sem):
    slots, bands = old_ref.shape[2:4]
    words, stations = bits_ref.shape[2], bits_ref.shape[4]
    column = lax.broadcasted_iota(jnp.int32, (stations, stations), 0)

    def write(s):
        return pltpu.make_async_copy(done.at[s], out_ref.at[0, 0, s], sem.at[s])

    for s in range(slots):
        code = codes[s]
        chosen = jnp.zeros((stations, stations), jnp.int32)
        bit = column
        for w in range(words):
            reached = column >= w * FLAG_BITS
            chosen = jnp.where(reached, bits_ref[0, s, w], chosen)
            bit = jnp.where(reached, column - w * FLAG_BITS, bit)
        flags = jnp.bitwise_and(jnp.right_shift(chosen, bit), 1).astype(jnp.float32).T > 0.5

        @pl.when(code == 0)
        def _():
            for k in range(bands):
                done[s, k] = old_ref[0, 0, s, k] + jnp.where(flags, self_ref[k], 0.0)

        @pl.when(code > 0)
        def _():
            for k in range(bands):
                done[s, k] = old_ref[0, 0, s, k] + jnp.where(
                    flags, c_ref[code - 1, k].astype(jnp.float32), 0.0)

        @pl.when(code < 0)
        def _():
            done[s] = old_ref[0, 0, s]

        write(s).start()
    for s in range(slots):
        write(s).wait()


def combine(codes, own, cross, range_bits, old):
    slots, bands, parts, stations = old.shape[2:6]
    vmem = pl.BlockSpec(memory_space=pltpu.VMEM)
    return pl.pallas_call(
        combine_kernel,
        out_shape=jax.ShapeDtypeStruct(old.shape, old.dtype),
        in_specs=[pl.BlockSpec(memory_space=pltpu.SMEM), vmem, vmem, vmem, vmem],
        out_specs=pl.BlockSpec(memory_space=pltpu.MemorySpace.HBM),
        scratch_shapes=[
            pltpu.VMEM((slots, bands, parts, stations, stations), jnp.float32),
            pltpu.SemaphoreType.DMA((slots,)),
        ],
        compiler_params=pltpu.CompilerParams(vmem_limit_bytes=20 * 1024 * 1024),
        name="combine",
    )(codes, own, cross, jnp.transpose(range_bits, (0, 2, 4, 1, 3)), old)


def solution(mesh):
    rows, cols = mesh.shape["gx"], mesh.shape["gy"]

    def body(spectra, partner_codes, range_bits, old_stacks):
        own, cross = crosses(spectra, old_stacks.shape[3], rows, cols)
        return combine(partner_codes[0, 0], own, cross, range_bits, old_stacks)

    return jax.shard_map(
        body,
        mesh=mesh,
        in_specs=(
            P("gx", "gy", None, None, None, None),
            P("gx", "gy", None),
            P("gx", "gy", None, None, None),
            P("gx", "gy", None, None, None, None, None),
        ),
        out_specs=P("gx", "gy", None, None, None, None, None),
        check_vma=False,
    )
```

```python
import functools
import math

import jax
import jax.numpy as jnp
from jax import lax
from jax.experimental import pallas as pl
from jax.experimental.pallas import tpu as pltpu
from jax.sharding import PartitionSpec as P

EPSILON = 1e-06
MESH = pl.DeviceIdType.MESH
FLAG_BITS = 30


def whiten_rows(ref, index, first, count):
    segments, parts, _, width = ref.shape[len(index):]
    chunk = 16

    def rows(i, _):
        at = pl.ds(pl.multiple_of(first + i * chunk, chunk), chunk)
        pieces = [ref[(*index, s, p, at)].astype(jnp.float32)
                  for s in range(segments) for p in range(parts)]
        total = pieces[0] * pieces[0]
        for v in pieces[1:]:
            total = total + v * v
        power = jnp.sum(total, axis=1, keepdims=True) * (1.0 / (len(pieces) * width))
        scale = lax.rsqrt(power + EPSILON)
        for s in range(segments):
            for p in range(parts):
                ref[(*index, s, p, at)] = (pieces[s * parts + p] * scale).astype(jnp.bfloat16)
        return 0

    lax.fori_loop(0, count // chunk, rows, 0, unroll=2)


def product(left, right, scale):
    segments = left.count
    total = None
    for s in range(segments):
        part = lax.dot_general(
            left(s), right(s), (((1,), (1,)), ((), ())), preferred_element_type=jnp.float32
        )
        total = part if total is None else total + part
    n = total.shape[0] // 2
    real = total[:n, :n] + total[n:, n:]
    imag = total[n:, :n] - total[:n, n:]
    return real * scale, imag * scale


class View:
    def __init__(self, ref, index, count):
        self.ref, self.index, self.count = ref, index, count

    def __call__(self, s):
        v = self.ref[(*self.index, s)]
        return v.reshape(v.shape[0] * v.shape[1], v.shape[2])


OTHER = 3
PIECES = 4
EARLY = 1
AHEAD = 4
ACROSS = (1, 5, 7)
ORDER = (1, 5, 7, 0, 4, 6, 2, 3)
GROUP = (3, 0, 6, 6, 4, 1, 5, 2)


def cross_kernel(rows, cols, x_ref, self_ref, c_ref, both, stage,
                 first_sem, load_sem, xs, xr, zs, zr, ms, mr, ks, kr, rs, rr):
    blk, far = both.at[0], both.at[1]
    half, segments, stations, width = both.shape[1], both.shape[3], both.shape[5], both.shape[6]
    scale = 1.0 / math.sqrt(segments * width)
    piece = stations // PIECES
    turns = [(half + 1 - parity) // 2 for parity in (0, 1)]
    r = lax.axis_index("gx")
    c = lax.axis_index("gy")
    odd = lax.rem(c, 2)
    mate = c + 1 - 2 * odd
    keep_slot = 2 * odd
    halo_slot = 2 - 2 * odd
    z_to = c - 2 + 4 * odd
    z_from = c + 2 - 4 * odd
    sends_z = (z_to >= 0) & (z_to < cols)
    has_halo = (z_from >= 0) & (z_from < cols)
    first_col = c - 2 * odd
    above = r > 0
    below = r + 1 < rows
    left_pair = (odd == 0) | has_halo
    right_pair = (odd == 1) | has_halo

    def strip(q):
        return pl.ds(q * piece if isinstance(q, int) else pl.multiple_of(q * piece, piece), piece)

    def bins(b, mine):
        band = half * (odd if mine else 1 - odd) + b
        return pl.ds(pl.multiple_of(band * width, width), width)

    def load(b, mine):
        slot = keep_slot if mine else OTHER
        return pltpu.make_async_copy(
            x_ref.at[0, 0, :, :, :, bins(b, mine)], blk.at[b, slot], load_sem.at[int(mine), b])

    def load_first(q):
        return pltpu.make_async_copy(
            x_ref.at[0, 0, :, :, strip(q), bins(0, False)], blk.at[0, OTHER, :, :, strip(q)],
            first_sem.at[q])

    def x_copy(b, q):
        return pltpu.make_async_remote_copy(
            src_ref=blk.at[b, OTHER, :, :, strip(q)], dst_ref=blk.at[b, 1, :, :, strip(q)],
            send_sem=xs.at[0], recv_sem=xr.at[b, q],
            device_id=(r, mate), device_id_type=MESH)

    def z_copy(b):
        return pltpu.make_async_remote_copy(
            src_ref=blk.at[b, keep_slot], dst_ref=blk.at[b, halo_slot],
            send_sem=zs.at[0], recv_sem=zr.at[b], device_id=(r, z_to), device_id_type=MESH)

    def mid_copy(b, q, d):
        return pltpu.make_async_remote_copy(
            src_ref=blk.at[b, 1, :, :, strip(q)], dst_ref=far.at[b, d, :, :, strip(q)],
            send_sem=ms.at[d], recv_sem=mr.at[b, d],
            device_id=(r + 1 - 2 * d, c), device_id_type=MESH)

    def side_to(parity):
        return r - 1 + 2 * parity

    def sides(parity):
        to = side_to(parity)
        return (to >= 0) & (to < rows)

    def meets(parity):
        other_row = r + 1 - 2 * parity
        return (other_row >= 0) & (other_row < rows)

    def side_copy(parity, step):
        b = 2 * (step // (2 * PIECES)) + parity
        e = lax.rem(step // PIECES, 2)
        q = lax.rem(step, PIECES)
        slot = keep_slot + e * (OTHER - keep_slot)
        return pltpu.make_async_remote_copy(
            src_ref=blk.at[b, slot, :, :, strip(q)], dst_ref=far.at[b, 2 + e, :, :, strip(q)],
            send_sem=ks.at[parity], recv_sem=kr.at[b],
            device_id=(side_to(parity), c), device_id_type=MESH)

    def whole(slots, send, recv):
        return pltpu.make_async_remote_copy(
            src_ref=slots, dst_ref=slots, send_sem=send, recv_sem=recv,
            device_id=(r, mate), device_id_type=MESH)

    def r_copy(b, which, code, band, row, col):
        return pltpu.make_async_remote_copy(
            src_ref=stage.at[b, which], dst_ref=c_ref.at[code - 1, band],
            send_sem=rs.at[GROUP[which]], recv_sem=rr.at[code - 1],
            device_id=(row, col), device_id_type=MESH)

    def results(count, send=0, code=1):
        return whole(c_ref.at[0, pl.ds(0, count)], rs.at[send], rr.at[code - 1])

    def load_band(b, _):
        pl.when(b > 0)(load(b, False).start)
        load(b, True).start()
        return 0

    def send_other(b):
        load(b, False).wait()
        whiten_rows(both, (0, b, OTHER), 0, stations)
        for q in range(PIECES):
            x_copy(b, q).start()

    def send_mine(b, _):
        load(b, True).wait()
        whiten_rows(both, (0, b, keep_slot), 0, stations)
        pl.when(sends_z)(z_copy(b).start)
        return 0

    for q in range(PIECES):
        load_first(q).start()
    barrier = pltpu.get_barrier_semaphore()
    peers = jnp.int32(0)
    for dr in (0, 1, -1):
        for col in (mate, c - 2, c + 2) if dr == 0 else (c, mate):
            there = (r + dr >= 0) & (r + dr < rows) & (col >= 0) & (col < cols)
            peers = peers + there.astype(jnp.int32)

            @pl.when(there)
            def _():
                pl.semaphore_signal(barrier, inc=1, device_id=(r + dr, col), device_id_type=MESH)
    lax.fori_loop(0, half, load_band, 0)
    for q in range(PIECES):
        load_first(q).wait()
        whiten_rows(both, (0, 0, OTHER), q * piece, piece)
        if q == 0:
            pl.semaphore_wait(barrier, peers)
        x_copy(0, q).start()
    lax.fori_loop(0, 2, send_mine, 0)
    for step in range(AHEAD):
        for parity in (0, 1):
            pl.when(sides(parity))(side_copy(parity, jnp.int32(step)).start)

    def send_rest(b, _):
        send_other(b)

        @pl.when(b > 1)
        def _():
            send_mine(b, 0)
        return 0

    lax.fori_loop(1, half, send_rest, 0)

    def own_product(b):
        for slot, band in ((keep_slot, half * odd + b), (OTHER, half * (1 - odd) + b)):
            view = View(both, (0, b, slot), segments)
            real, imag = product(view, view, scale)
            self_ref[band, 0] = real
            self_ref[band, 1] = imag

    def routes(b):
        is_odd = lax.rem(b, 2)
        even = is_odd == 0
        band, other_band = half * odd + b, half * (1 - odd) + b
        near = odd == 0
        left, mid, right = (0, b, 0), (0, b, 1), (0, b, 2)
        mid_above, mid_below = (1, b, 0), (1, b, 1)
        keeps = (is_odd, b, keep_slot + is_odd * (2 - keep_slot)), (1 - is_odd, b, 2 + is_odd * (keep_slot - 2))
        return [
            (0, left, mid, 3, band, r, first_col, left_pair, near),
            (1, mid, right, 3, band, r, mate, right_pair, None),
            (2, *keeps, 1, band, r - is_odd, c, meets(is_odd), even),
            (3, (is_odd, b, OTHER), (1 - is_odd, b, OTHER), 1, other_band, r - is_odd, c, meets(is_odd), even),
            (4, left, mid_below, 4, band, r, first_col, below & left_pair, near),
            (5, mid_above, right, 4, band, r - 1, mate, above & right_pair, None),
            (6, left, mid_above, 2, band, r, first_col, above & left_pair, near),
            (7, mid_below, right, 2, band, r + 1, mate, below & right_pair, None),
        ]

    def emit(b, route, go=True):
        which, left, right, code, band, row, col, present, local = route

        @pl.when(present)
        def _():
            real, imag = product(View(both, left, segments), View(both, right, segments), scale)
            real, imag = real.astype(jnp.bfloat16), imag.astype(jnp.bfloat16)

            def remote():
                stage[b, which, 0] = real
                stage[b, which, 1] = imag
                pl.when(go)(r_copy(b, which, code, band, row, col).start)

            if local is None:
                remote()
            else:
                @pl.when(local)
                def _():
                    c_ref[code - 1, band, 0] = real
                    c_ref[code - 1, band, 1] = imag

                pl.when(jnp.logical_not(local))(remote)

    last = jnp.where(lax.rem(r, 2) == 0, 1, jnp.where((r == 1) & (c == 1), 7, 5))

    def fire(a, held):
        table = routes(a)
        for which in ACROSS:
            _, _, _, code, band, row, col, present, _ = table[which]
            turn = (last == which) == held
            pl.when(present & turn)(r_copy(a, which, code, band, row, col).start)

    def step(b, _):
        for q in range(PIECES):
            @pl.when(b < half)
            def _():
                if q == 3:
                    @pl.when(b == half - 1)
                    def _():
                        for a in range(half - 1):
                            fire(a, False)
                        for a in range(EARLY):
                            fire(a, True)
                x_copy(b, q).wait_recv()
                for d, there in ((0, below), (1, above)):
                    pl.when(there)(mid_copy(b, q, d).start)
                at = b * PIECES + q + AHEAD
                for parity in (0, 1):
                    pl.when(sides(parity) & (at < 2 * PIECES * turns[parity]))(side_copy(parity, at).start)

            @pl.when(b == 0)
            def _():
                for a in range(q, half, PIECES):
                    own_product(a)

            @pl.when(b > 0)
            def _():
                a = b - 1
                table = routes(a)
                for which in ORDER[2 * q: 2 * q + 2]:
                    if which == 1:
                        pl.when(has_halo)(z_copy(a).wait_recv)
                    if which == 5:
                        pl.when(above)(whole(far.at[a, 0], ms.at[0], mr.at[a, 0]).wait_recv)
                    if which == 7:
                        pl.when(below)(whole(far.at[a, 1], ms.at[0], mr.at[a, 1]).wait_recv)
                    if which == 2:
                        pl.when(meets(lax.rem(a, 2)))(
                            whole(far.at[a, pl.ds(2, 2)], ks.at[0], kr.at[a]).wait_recv)
                    emit(a, table[which], (a == half - 1) & (last != which) if which in ACROSS else True)
                    if which == 7:
                        @pl.when(a == half - 1)
                        def _():
                            for e in range(EARLY, half):
                                fire(e, True)
        return 0

    lax.fori_loop(0, half + 1, step, 0)

    whole(blk.at[:, OTHER], xs.at[0], xr.at[0, 0]).wait_send()
    pl.when(sends_z)(whole(blk.at[:, OTHER], zs.at[0], xr.at[0, 0]).wait_send)
    for d, there in ((0, below), (1, above)):
        pl.when(there)(whole(blk.at[:, 1], ms.at[d], xr.at[0, 0]).wait_send)
    for parity in (0, 1):
        pl.when(sides(parity))(
            whole(far.at[pl.ds(0, turns[parity]), pl.ds(2, 2)], ks.at[parity], xr.at[0, 0]).wait_send)
    for group, there in enumerate((right_pair, above & right_pair, below & right_pair)):
        pl.when(there)(results(half, group).wait_send)
    for group, there in enumerate((left_pair, below & left_pair, above & left_pair), 3):
        pl.when(there & (odd == 1))(results(half, group).wait_send)
    pl.when(meets(1))(results(2 * turns[1], 6).wait_send)

    next_col = c + 1 < cols
    pl.when(below)(results(2 * turns[1], code=1).wait_recv)
    for code, comes in ((2, above & next_col), (3, next_col), (4, below & next_col)):
        pl.when(comes & (odd == 1))(results(2 * half, code=code).wait_recv)
        pl.when(comes & (odd == 0))(results(half, code=code).wait_recv)


def crosses(spectra, bands, rows, cols):
    segments, parts, stations, bins = spectra.shape[2:]
    half, width = bands // 2, bins // bands
    dma = pltpu.SemaphoreType.DMA
    return pl.pallas_call(
        functools.partial(cross_kernel, rows, cols),
        out_shape=(
            jax.ShapeDtypeStruct((bands, 2, stations, stations), jnp.float32),
            jax.ShapeDtypeStruct((4, bands, 2, stations, stations), jnp.bfloat16),
        ),
        in_specs=[pl.BlockSpec(memory_space=pltpu.MemorySpace.HBM)],
        out_specs=(pl.BlockSpec(memory_space=pltpu.VMEM), pl.BlockSpec(memory_space=pltpu.VMEM)),
        scratch_shapes=[
            pltpu.VMEM((2, half, 4, segments, parts, stations, width), jnp.bfloat16),
            pltpu.VMEM((half, 8, 2, stations, stations), jnp.bfloat16),
            dma((PIECES,)), dma((2, half)),
            dma((1,)), dma((half, PIECES)),
            dma((1,)), dma((half,)),
            dma((2,)), dma((half, 2)),
            dma((2,)), dma((half,)),
            dma((7,)), dma((4,)),
        ],
        compiler_params=pltpu.CompilerParams(collective_id=0, has_side_effects=True, vmem_limit_bytes=48 * 1024 * 1024),
        name="crosses",
    )(spectra)


def combine_kernel(codes_ref, self_ref, c_ref, bits_ref, old_ref, out_ref, done, flags_ref, codes, code_sem, sem):
    slots, bands = old_ref.shape[2:4]
    words, stations = bits_ref.shape[2], bits_ref.shape[4]
    column = lax.broadcasted_iota(jnp.int32, (stations, stations), 0)
    span = bands // 2

    def write(s, first=0, count=bands):
        at = pl.ds(first, count)
        return pltpu.make_async_copy(done.at[s, at], out_ref.at[0, 0, s, at], sem)

    def near(s):
        chosen = jnp.zeros((stations, stations), jnp.int32)
        bit = column
        for w in range(words):
            reached = column >= w * FLAG_BITS
            chosen = jnp.where(reached, bits_ref[0, s, w], chosen)
            bit = jnp.where(reached, column - w * FLAG_BITS, bit)
        return jnp.bitwise_and(jnp.right_shift(chosen, bit), 1).astype(jnp.float32).T > 0.5

    fetch = pltpu.make_async_copy(codes_ref, codes, code_sem)
    fetch.start()
    flags = near(0)
    for h in range(2):
        def own(k, _):
            done[0, k] = old_ref[0, 0, 0, k] + jnp.where(flags, self_ref[k], 0.0)
            return 0

        lax.fori_loop(h * span, (h + 1) * span, own, 0)
        write(0, h * span, span).start()

    def unpack(s, _):
        flags_ref[s] = near(s).astype(jnp.float32)
        return 0

    lax.fori_loop(1, slots, unpack, 0)
    fetch.wait()

    def slot(s, _):
        code = codes[s]
        flags = (flags_ref[s] > 0.5) & (code > 0)
        at = jnp.maximum(code - 1, 0)

        def band(k, _):
            done[s, k] = old_ref[0, 0, s, k] + jnp.where(flags, c_ref[at, k].astype(jnp.float32), 0.0)
            return 0

        lax.fori_loop(0, bands, band, 0)
        write(s).start()
        return 0

    lax.fori_loop(1, slots, slot, 0)
    pltpu.make_async_copy(done, out_ref.at[0, 0], sem).wait()


def combine(codes, own, cross, range_bits, old):
    slots, bands, parts, stations = old.shape[2:6]
    vmem = pl.BlockSpec(memory_space=pltpu.VMEM)
    return pl.pallas_call(
        combine_kernel,
        out_shape=jax.ShapeDtypeStruct(old.shape, old.dtype),
        in_specs=[vmem] * 5,
        out_specs=pl.BlockSpec(memory_space=pltpu.MemorySpace.HBM),
        scratch_shapes=[
            pltpu.VMEM((slots, bands, parts, stations, stations), jnp.float32),
            pltpu.VMEM((slots, stations, stations), jnp.float32),
            pltpu.SMEM(codes.shape, jnp.int32),
            pltpu.SemaphoreType.DMA(()),
            pltpu.SemaphoreType.DMA(()),
        ],
        compiler_params=pltpu.CompilerParams(vmem_limit_bytes=20 * 1024 * 1024),
        name="combine",
    )(codes, own, cross, jnp.transpose(range_bits, (0, 2, 4, 1, 3)), old)


def solution(mesh):
    rows, cols = mesh.shape["gx"], mesh.shape["gy"]

    def body(spectra, partner_codes, range_bits, old_stacks):
        own, cross = crosses(spectra, old_stacks.shape[3], rows, cols)
        return combine(partner_codes[0, 0], own, cross, range_bits, old_stacks)

    return jax.shard_map(
        body,
        mesh=mesh,
        in_specs=(
            P("gx", "gy", None, None, None, None),
            P("gx", "gy", None),
            P("gx", "gy", None, None, None),
            P("gx", "gy", None, None, None, None, None),
        ),
        out_specs=P("gx", "gy", None, None, None, None, None),
        check_vma=False,
    )
```

```python
import functools
import math

import jax
import jax.numpy as jnp
from jax import lax
from jax.experimental import pallas as pl
from jax.experimental.pallas import tpu as pltpu
from jax.sharding import PartitionSpec as P

EPSILON = 1e-06
MESH = pl.DeviceIdType.MESH
FLAG_BITS = 30


def whiten_rows(ref, index, first, count):
    segments, parts, _, width = ref.shape[len(index):]
    chunk = 16

    def rows(i, _):
        at = pl.ds(pl.multiple_of(first + i * chunk, chunk), chunk)
        pieces = [ref[(*index, s, p, at)].astype(jnp.float32)
                  for s in range(segments) for p in range(parts)]
        total = pieces[0] * pieces[0]
        for v in pieces[1:]:
            total = total + v * v
        power = jnp.sum(total, axis=1, keepdims=True) * (1.0 / (len(pieces) * width))
        scale = lax.rsqrt(power + EPSILON)
        for s in range(segments):
            for p in range(parts):
                ref[(*index, s, p, at)] = (pieces[s * parts + p] * scale).astype(jnp.bfloat16)
        return 0

    lax.fori_loop(0, count // chunk, rows, 0, unroll=2)


def product(left, right, scale):
    segments = left.count
    total = None
    for s in range(segments):
        part = lax.dot_general(
            left(s), right(s), (((1,), (1,)), ((), ())), preferred_element_type=jnp.float32
        )
        total = part if total is None else total + part
    n = total.shape[0] // 2
    real = total[:n, :n] + total[n:, n:]
    imag = total[n:, :n] - total[:n, n:]
    return real * scale, imag * scale


class View:
    def __init__(self, ref, index, count):
        self.ref, self.index, self.count = ref, index, count

    def __call__(self, s):
        v = self.ref[(*self.index, s)]
        return v.reshape(v.shape[0] * v.shape[1], v.shape[2])


OTHER = 3
PIECES = 4
EARLY = 1
AHEAD = 4
ACROSS = (1, 5, 7)
ORDER = (1, 5, 7, 0, 4, 6, 2, 3)
GROUP = (3, 0, 6, 6, 4, 1, 5, 2)


def codes_of(slot):
    return range(slot, 5) if slot else ()


def place(slot, code):
    return 1 + sum(len(codes_of(s)) for s in range(slot)) + code - slot


def cross_kernel(rows, cols, x_ref, codes_ref, bits_ref, old_ref, own_ref, chosen_ref, c_ref, both, stage,
                 bits, codes, side_sem, first_sem, load_sem, xs, xr, zs, zr, ms, mr, ks, kr, rs, rr):
    blk, far = both.at[0], both.at[1]
    half, segments, stations, width = both.shape[1], both.shape[3], both.shape[5], both.shape[6]
    scale = 1.0 / math.sqrt(segments * width)
    piece = stations // PIECES
    turns = [(half + 1 - parity) // 2 for parity in (0, 1)]
    r = lax.axis_index("gx")
    c = lax.axis_index("gy")
    odd = lax.rem(c, 2)
    mate = c + 1 - 2 * odd
    keep_slot = 2 * odd
    halo_slot = 2 - 2 * odd
    z_to = c - 2 + 4 * odd
    z_from = c + 2 - 4 * odd
    sends_z = (z_to >= 0) & (z_to < cols)
    has_halo = (z_from >= 0) & (z_from < cols)
    first_col = c - 2 * odd
    above = r > 0
    below = r + 1 < rows
    left_pair = (odd == 0) | has_halo
    right_pair = (odd == 1) | has_halo

    def strip(q):
        return pl.ds(q * piece if isinstance(q, int) else pl.multiple_of(q * piece, piece), piece)

    def bins(b, mine):
        band = half * (odd if mine else 1 - odd) + b
        return pl.ds(pl.multiple_of(band * width, width), width)

    def load(b, mine):
        slot = keep_slot if mine else OTHER
        return pltpu.make_async_copy(
            x_ref.at[0, 0, :, :, :, bins(b, mine)], blk.at[b, slot], load_sem.at[int(mine), b])

    def load_first(q):
        return pltpu.make_async_copy(
            x_ref.at[0, 0, :, :, strip(q), bins(0, False)], blk.at[0, OTHER, :, :, strip(q)],
            first_sem.at[q])

    def x_copy(b, q):
        return pltpu.make_async_remote_copy(
            src_ref=blk.at[b, OTHER, :, :, strip(q)], dst_ref=blk.at[b, 1, :, :, strip(q)],
            send_sem=xs.at[0], recv_sem=xr.at[b, q],
            device_id=(r, mate), device_id_type=MESH)

    def z_copy(b):
        return pltpu.make_async_remote_copy(
            src_ref=blk.at[b, keep_slot], dst_ref=blk.at[b, halo_slot],
            send_sem=zs.at[0], recv_sem=zr.at[b], device_id=(r, z_to), device_id_type=MESH)

    def mid_copy(b, q, d):
        return pltpu.make_async_remote_copy(
            src_ref=blk.at[b, 1, :, :, strip(q)], dst_ref=far.at[b, d, :, :, strip(q)],
            send_sem=ms.at[d], recv_sem=mr.at[b, d],
            device_id=(r + 1 - 2 * d, c), device_id_type=MESH)

    def side_to(parity):
        return r - 1 + 2 * parity

    def sides(parity):
        to = side_to(parity)
        return (to >= 0) & (to < rows)

    def meets(parity):
        other_row = r + 1 - 2 * parity
        return (other_row >= 0) & (other_row < rows)

    def side_copy(parity, step):
        b = 2 * (step // (2 * PIECES)) + parity
        e = lax.rem(step // PIECES, 2)
        q = lax.rem(step, PIECES)
        slot = keep_slot + e * (OTHER - keep_slot)
        return pltpu.make_async_remote_copy(
            src_ref=blk.at[b, slot, :, :, strip(q)], dst_ref=far.at[b, 2 + e, :, :, strip(q)],
            send_sem=ks.at[parity], recv_sem=kr.at[b],
            device_id=(side_to(parity), c), device_id_type=MESH)

    def whole(slots, send, recv):
        return pltpu.make_async_remote_copy(
            src_ref=slots, dst_ref=slots, send_sem=send, recv_sem=recv,
            device_id=(r, mate), device_id_type=MESH)

    def r_copy(b, which, code, band, row, col):
        return pltpu.make_async_remote_copy(
            src_ref=stage.at[b, which], dst_ref=c_ref.at[code - 1, band],
            send_sem=rs.at[GROUP[which]], recv_sem=rr.at[code - 1],
            device_id=(row, col), device_id_type=MESH)

    def results(count, send=0, code=1):
        return whole(c_ref.at[0, pl.ds(0, count)], rs.at[send], rr.at[code - 1])

    def load_codes():
        return pltpu.make_async_copy(codes_ref, codes, side_sem.at[0])

    def load_bits():
        return pltpu.make_async_copy(bits_ref.at[0], bits, side_sem.at[1])

    def load_old():
        return pltpu.make_async_copy(old_ref.at[0, 0, 0], own_ref, side_sem.at[2])

    def unpack():
        column = lax.broadcasted_iota(jnp.int32, (stations, stations), 0)
        load_bits().wait()
        load_codes().wait()
        for s in range(bits.shape[0]):
            word = jnp.zeros((stations, stations), jnp.int32)
            bit = column
            for w in range(bits.shape[1]):
                reached = column >= w * FLAG_BITS
                word = jnp.where(reached, bits[s, w], word)
                bit = jnp.where(reached, column - w * FLAG_BITS, bit)
            near = jnp.bitwise_and(jnp.right_shift(word, bit), 1).astype(jnp.float32).T
            if s == 0:
                chosen_ref[0] = near
            for code in codes_of(s):
                chosen_ref[place(s, code)] = near * jnp.where(codes[s] == code, 1.0, 0.0)

    def load_band(b, _):
        pl.when(b > 0)(load(b, False).start)
        load(b, True).start()
        return 0

    def send_other(b):
        load(b, False).wait()
        whiten_rows(both, (0, b, OTHER), 0, stations)
        for q in range(PIECES):
            x_copy(b, q).start()

    def send_mine(b, _):
        load(b, True).wait()
        whiten_rows(both, (0, b, keep_slot), 0, stations)
        pl.when(sends_z)(z_copy(b).start)
        return 0

    for q in range(PIECES):
        load_first(q).start()
    barrier = pltpu.get_barrier_semaphore()
    peers = jnp.int32(0)
    for dr in (0, 1, -1):
        for col in (mate, c - 2, c + 2) if dr == 0 else (c, mate):
            there = (r + dr >= 0) & (r + dr < rows) & (col >= 0) & (col < cols)
            peers = peers + there.astype(jnp.int32)

            @pl.when(there)
            def _():
                pl.semaphore_signal(barrier, inc=1, device_id=(r + dr, col), device_id_type=MESH)
    lax.fori_loop(0, half, load_band, 0)
    load_codes().start()
    load_bits().start()
    load_old().start()
    for q in range(PIECES):
        load_first(q).wait()
        whiten_rows(both, (0, 0, OTHER), q * piece, piece)
        if q == 0:
            pl.semaphore_wait(barrier, peers)
        x_copy(0, q).start()
    lax.fori_loop(0, 2, send_mine, 0)
    for step in range(AHEAD):
        for parity in (0, 1):
            pl.when(sides(parity))(side_copy(parity, jnp.int32(step)).start)

    def send_rest(b, _):
        send_other(b)

        @pl.when(b > 1)
        def _():
            send_mine(b, 0)
        return 0

    lax.fori_loop(1, half, send_rest, 0)

    def own_product(b):
        for slot, band in ((keep_slot, half * odd + b), (OTHER, half * (1 - odd) + b)):
            view = View(both, (0, b, slot), segments)
            real, imag = product(view, view, scale)
            near = chosen_ref[0] > 0.5
            own_ref[band, 0] += jnp.where(near, real, 0.0)
            own_ref[band, 1] += jnp.where(near, imag, 0.0)

    def routes(b):
        is_odd = lax.rem(b, 2)
        even = is_odd == 0
        band, other_band = half * odd + b, half * (1 - odd) + b
        near = odd == 0
        left, mid, right = (0, b, 0), (0, b, 1), (0, b, 2)
        mid_above, mid_below = (1, b, 0), (1, b, 1)
        keeps = (is_odd, b, keep_slot + is_odd * (2 - keep_slot)), (1 - is_odd, b, 2 + is_odd * (keep_slot - 2))
        return [
            (0, left, mid, 3, band, r, first_col, left_pair, near),
            (1, mid, right, 3, band, r, mate, right_pair, None),
            (2, *keeps, 1, band, r - is_odd, c, meets(is_odd), even),
            (3, (is_odd, b, OTHER), (1 - is_odd, b, OTHER), 1, other_band, r - is_odd, c, meets(is_odd), even),
            (4, left, mid_below, 4, band, r, first_col, below & left_pair, near),
            (5, mid_above, right, 4, band, r - 1, mate, above & right_pair, None),
            (6, left, mid_above, 2, band, r, first_col, above & left_pair, near),
            (7, mid_below, right, 2, band, r + 1, mate, below & right_pair, None),
        ]

    def emit(b, route, go=True):
        which, left, right, code, band, row, col, present, local = route

        @pl.when(present)
        def _():
            real, imag = product(View(both, left, segments), View(both, right, segments), scale)
            real, imag = real.astype(jnp.bfloat16), imag.astype(jnp.bfloat16)

            def remote():
                stage[b, which, 0] = real
                stage[b, which, 1] = imag
                pl.when(go)(r_copy(b, which, code, band, row, col).start)

            if local is None:
                remote()
            else:
                @pl.when(local)
                def _():
                    c_ref[code - 1, band, 0] = real
                    c_ref[code - 1, band, 1] = imag

                pl.when(jnp.logical_not(local))(remote)

    last = jnp.where(lax.rem(r, 2) == 0, 1, jnp.where((r == 1) & (c == 1), 7, 5))

    def fire(a, held):
        table = routes(a)
        for which in ACROSS:
            _, _, _, code, band, row, col, present, _ = table[which]
            turn = (last == which) == held
            pl.when(present & turn)(r_copy(a, which, code, band, row, col).start)

    def step(b, _):
        for q in range(PIECES):
            @pl.when(b < half)
            def _():
                if q == 3:
                    @pl.when(b == half - 1)
                    def _():
                        for a in range(half - 1):
                            fire(a, False)
                        for a in range(EARLY):
                            fire(a, True)
                x_copy(b, q).wait_recv()
                for d, there in ((0, below), (1, above)):
                    pl.when(there)(mid_copy(b, q, d).start)
                at = b * PIECES + q + AHEAD
                for parity in (0, 1):
                    pl.when(sides(parity) & (at < 2 * PIECES * turns[parity]))(side_copy(parity, at).start)

            @pl.when(b == 0)
            def _():
                for a in range(q, half, PIECES):
                    own_product(a)

            @pl.when(b > 0)
            def _():
                a = b - 1
                table = routes(a)
                for which in ORDER[2 * q: 2 * q + 2]:
                    if which == 1:
                        pl.when(has_halo)(z_copy(a).wait_recv)
                    if which == 5:
                        pl.when(above)(whole(far.at[a, 0], ms.at[0], mr.at[a, 0]).wait_recv)
                    if which == 7:
                        pl.when(below)(whole(far.at[a, 1], ms.at[0], mr.at[a, 1]).wait_recv)
                    if which == 2:
                        pl.when(meets(lax.rem(a, 2)))(
                            whole(far.at[a, pl.ds(2, 2)], ks.at[0], kr.at[a]).wait_recv)
                    emit(a, table[which], (a == half - 1) & (last != which) if which in ACROSS else True)
                    if which == 7:
                        @pl.when(a == half - 1)
                        def _():
                            for e in range(EARLY, half):
                                fire(e, True)
        return 0

    unpack()
    load_old().wait()
    lax.fori_loop(0, half + 1, step, 0)

    whole(blk.at[:, OTHER], xs.at[0], xr.at[0, 0]).wait_send()
    pl.when(sends_z)(whole(blk.at[:, OTHER], zs.at[0], xr.at[0, 0]).wait_send)
    for d, there in ((0, below), (1, above)):
        pl.when(there)(whole(blk.at[:, 1], ms.at[d], xr.at[0, 0]).wait_send)
    for parity in (0, 1):
        pl.when(sides(parity))(
            whole(far.at[pl.ds(0, turns[parity]), pl.ds(2, 2)], ks.at[parity], xr.at[0, 0]).wait_send)
    for group, there in enumerate((right_pair, above & right_pair, below & right_pair)):
        pl.when(there)(results(half, group).wait_send)
    for group, there in enumerate((left_pair, below & left_pair, above & left_pair), 3):
        pl.when(there & (odd == 1))(results(half, group).wait_send)
    pl.when(meets(1))(results(2 * turns[1], 6).wait_send)

    next_col = c + 1 < cols
    pl.when(below)(results(2 * turns[1], code=1).wait_recv)
    for code, comes in ((2, above & next_col), (3, next_col), (4, below & next_col)):
        pl.when(comes & (odd == 1))(results(2 * half, code=code).wait_recv)
        pl.when(comes & (odd == 0))(results(half, code=code).wait_recv)


def crosses(spectra, codes, range_bits, old, rows, cols):
    segments, parts, stations, bins = spectra.shape[2:]
    slots, bands, words = old.shape[2], old.shape[3], range_bits.shape[4]
    half, width = bands // 2, bins // bands
    hbm = pl.BlockSpec(memory_space=pltpu.MemorySpace.HBM)
    vmem = pl.BlockSpec(memory_space=pltpu.VMEM)
    bits = jnp.transpose(range_bits, (0, 2, 4, 1, 3))
    dma = pltpu.SemaphoreType.DMA
    return pl.pallas_call(
        functools.partial(cross_kernel, rows, cols),
        out_shape=(
            jax.ShapeDtypeStruct((bands, 2, stations, stations), jnp.float32),
            jax.ShapeDtypeStruct((place(slots, slots), stations, stations), jnp.float32),
            jax.ShapeDtypeStruct((4, bands, 2, stations, stations), jnp.bfloat16),
        ),
        in_specs=[hbm] * 4,
        out_specs=(vmem, vmem, vmem),
        scratch_shapes=[
            pltpu.VMEM((2, half, 4, segments, parts, stations, width), jnp.bfloat16),
            pltpu.VMEM((half, 8, 2, stations, stations), jnp.bfloat16),
            pltpu.VMEM((slots, words, 1, stations), jnp.int32),
            pltpu.SMEM(codes.shape, jnp.int32),
            dma((3,)), dma((PIECES,)), dma((2, half)),
            dma((1,)), dma((half, PIECES)),
            dma((1,)), dma((half,)),
            dma((2,)), dma((half, 2)),
            dma((2,)), dma((half,)),
            dma((7,)), dma((4,)),
        ],
        compiler_params=pltpu.CompilerParams(collective_id=0, has_side_effects=True, vmem_limit_bytes=48 * 1024 * 1024),
        name="crosses",
    )(
        spectra,
        pltpu.with_memory_space_constraint(codes, pltpu.HBM),
        pltpu.with_memory_space_constraint(bits, pltpu.HBM),
        old,
    )


def combine_kernel(own_ref, chosen_ref, c_ref, old_ref, out_ref, done, own_sem, sem):
    slots, bands = old_ref.shape[2:4]
    own = pltpu.make_async_copy(own_ref, out_ref.at[0, 0, 0], own_sem)
    own.start()
    for s in reversed(range(1, slots)):
        def band(k, _):
            total = old_ref[0, 0, s, k]
            for code in codes_of(s):
                near = chosen_ref[place(s, code)] > 0.5
                total = total + jnp.where(near, c_ref[code - 1, k].astype(jnp.float32), 0.0)
            done[s - 1, k] = total
            return 0

        lax.fori_loop(0, bands, band, 0)
        pltpu.make_async_copy(done.at[s - 1], out_ref.at[0, 0, s], sem).start()
    own.wait()
    pltpu.make_async_copy(done, out_ref.at[0, 0, pl.ds(1, slots - 1)], sem).wait()


def combine(own, chosen, cross, old):
    slots, bands, parts, stations = old.shape[2:6]
    return pl.pallas_call(
        combine_kernel,
        out_shape=jax.ShapeDtypeStruct(old.shape, old.dtype),
        in_specs=[pl.BlockSpec(memory_space=pltpu.VMEM)] * 4,
        out_specs=pl.BlockSpec(memory_space=pltpu.MemorySpace.HBM),
        scratch_shapes=[
            pltpu.VMEM((slots - 1, bands, parts, stations, stations), jnp.float32),
            pltpu.SemaphoreType.DMA(()),
            pltpu.SemaphoreType.DMA(()),
        ],
        compiler_params=pltpu.CompilerParams(vmem_limit_bytes=16 * 1024 * 1024),
        name="combine",
    )(own, chosen, cross, old)


def solution(mesh):
    rows, cols = mesh.shape["gx"], mesh.shape["gy"]

    def body(spectra, partner_codes, range_bits, old_stacks):
        own, chosen, cross = crosses(spectra, partner_codes[0, 0], range_bits, old_stacks, rows, cols)
        return combine(own, chosen, cross, old_stacks)

    return jax.shard_map(
        body,
        mesh=mesh,
        in_specs=(
            P("gx", "gy", None, None, None, None),
            P("gx", "gy", None),
            P("gx", "gy", None, None, None),
            P("gx", "gy", None, None, None, None, None),
        ),
        out_specs=P("gx", "gy", None, None, None, None, None),
        check_vma=False,
    )
```

```python
import functools
import math

import jax
import jax.numpy as jnp
from jax import lax
from jax.experimental import pallas as pl
from jax.experimental.pallas import tpu as pltpu
from jax.sharding import PartitionSpec as P

EPSILON = 1e-06
MESH = pl.DeviceIdType.MESH
FLAG_BITS = 30


def whiten_rows(ref, index, first, count):
    segments, parts, _, width = ref.shape[len(index):]
    chunk = 16

    def rows(i, _):
        at = pl.ds(pl.multiple_of(first + i * chunk, chunk), chunk)
        pieces = [ref[(*index, s, p, at)].astype(jnp.float32)
                  for s in range(segments) for p in range(parts)]
        total = pieces[0] * pieces[0]
        for v in pieces[1:]:
            total = total + v * v
        power = jnp.sum(total, axis=1, keepdims=True) * (1.0 / (len(pieces) * width))
        scale = lax.rsqrt(power + EPSILON)
        for s in range(segments):
            for p in range(parts):
                ref[(*index, s, p, at)] = (pieces[s * parts + p] * scale).astype(jnp.bfloat16)
        return 0

    lax.fori_loop(0, count // chunk, rows, 0, unroll=2)


def product(left, right, scale):
    segments = left.count
    total = None
    for s in range(segments):
        part = lax.dot_general(
            left(s), right(s), (((1,), (1,)), ((), ())), preferred_element_type=jnp.float32
        )
        total = part if total is None else total + part
    n = total.shape[0] // 2
    real = total[:n, :n] + total[n:, n:]
    imag = total[n:, :n] - total[:n, n:]
    return real * scale, imag * scale


class View:
    def __init__(self, ref, index, count):
        self.ref, self.index, self.count = ref, index, count

    def __call__(self, s):
        v = self.ref[(*self.index, s)]
        return v.reshape(v.shape[0] * v.shape[1], v.shape[2])


OTHER = 3
PIECES = 4
EARLY = 1
AHEAD = 8
ACROSS = (1, 5, 7)
ORDER = (1, 5, 7, 0, 4, 6, 2, 3)
GROUP = (3, 0, 6, 6, 4, 1, 5, 2)


def codes_of(slot):
    return range(slot, 5) if slot else ()


def place(slot, code):
    return 1 + sum(len(codes_of(s)) for s in range(slot)) + code - slot


def cross_kernel(rows, cols, x_ref, codes_ref, bits_ref, old_ref, own_ref, chosen_ref, c_ref, both, stage,
                 bits, codes, first_sem, load_sem, xs, xr, zs, zr, ms, mr, kr, rs, rr):
    blk, far = both.at[0], both.at[1]
    half, segments, stations, width = both.shape[1], both.shape[3], both.shape[5], both.shape[6]
    scale = 1.0 / math.sqrt(segments * width)
    piece = stations // PIECES
    turns = [(half + 1 - parity) // 2 for parity in (0, 1)]
    r = lax.axis_index("gx")
    c = lax.axis_index("gy")
    odd = lax.rem(c, 2)
    mate = c + 1 - 2 * odd
    keep_slot = 2 * odd
    halo_slot = 2 - 2 * odd
    z_to = c - 2 + 4 * odd
    z_from = c + 2 - 4 * odd
    sends_z = (z_to >= 0) & (z_to < cols)
    has_halo = (z_from >= 0) & (z_from < cols)
    first_col = c - 2 * odd
    above = r > 0
    below = r + 1 < rows
    left_pair = (odd == 0) | has_halo
    right_pair = (odd == 1) | has_halo

    def strip(q):
        return pl.ds(q * piece if isinstance(q, int) else pl.multiple_of(q * piece, piece), piece)

    def bins(b, mine):
        band = half * (odd if mine else 1 - odd) + b
        return pl.ds(pl.multiple_of(band * width, width), width)

    def load(b, mine):
        slot = keep_slot if mine else OTHER
        return pltpu.make_async_copy(
            x_ref.at[0, 0, :, :, :, bins(b, mine)], blk.at[b, slot], load_sem.at[b])

    def load_first(q):
        return pltpu.make_async_copy(
            x_ref.at[0, 0, :, :, strip(q), bins(0, False)], blk.at[0, OTHER, :, :, strip(q)],
            first_sem.at[q])

    def x_copy(b, q):
        return pltpu.make_async_remote_copy(
            src_ref=blk.at[b, OTHER, :, :, strip(q)], dst_ref=blk.at[b, 1, :, :, strip(q)],
            send_sem=xs.at[0], recv_sem=xr.at[b, q],
            device_id=(r, mate), device_id_type=MESH)

    def z_copy(b):
        return pltpu.make_async_remote_copy(
            src_ref=blk.at[b, keep_slot], dst_ref=blk.at[b, halo_slot],
            send_sem=zs.at[0], recv_sem=zr.at[b], device_id=(r, z_to), device_id_type=MESH)

    def mid_copy(b, q, d):
        return pltpu.make_async_remote_copy(
            src_ref=blk.at[b, 1, :, :, strip(q)], dst_ref=far.at[b, d, :, :, strip(q)],
            send_sem=ms.at[d], recv_sem=mr.at[b, d],
            device_id=(r + 1 - 2 * d, c), device_id_type=MESH)

    def side_to(parity):
        return r - 1 + 2 * parity

    def sides(parity):
        to = side_to(parity)
        return (to >= 0) & (to < rows)

    def meets(parity):
        other_row = r + 1 - 2 * parity
        return (other_row >= 0) & (other_row < rows)

    def side_copy(parity, step):
        b = 2 * (step // (2 * PIECES)) + parity
        e = lax.rem(step // PIECES, 2)
        q = lax.rem(step, PIECES)
        slot = keep_slot + e * (OTHER - keep_slot)
        return pltpu.make_async_remote_copy(
            src_ref=blk.at[b, slot, :, :, strip(q)], dst_ref=far.at[b, 2 + e, :, :, strip(q)],
            send_sem=ms.at[1 - parity], recv_sem=kr.at[b],
            device_id=(side_to(parity), c), device_id_type=MESH)

    def whole(slots, send, recv):
        return pltpu.make_async_remote_copy(
            src_ref=slots, dst_ref=slots, send_sem=send, recv_sem=recv,
            device_id=(r, mate), device_id_type=MESH)

    def r_copy(b, which, code, band, row, col):
        return pltpu.make_async_remote_copy(
            src_ref=stage.at[b, which], dst_ref=c_ref.at[code - 1, band],
            send_sem=rs.at[GROUP[which]], recv_sem=rr.at[code - 1],
            device_id=(row, col), device_id_type=MESH)

    def results(count, send=0, code=1):
        return whole(c_ref.at[0, pl.ds(0, count)], rs.at[send], rr.at[code - 1])

    def load_codes():
        return pltpu.make_async_copy(codes_ref, codes, first_sem.at[0])

    def load_bits():
        return pltpu.make_async_copy(bits_ref.at[0], bits, first_sem.at[1])

    def load_old():
        return pltpu.make_async_copy(old_ref.at[0, 0, 0], own_ref, first_sem.at[2])

    def unpack():
        column = lax.broadcasted_iota(jnp.int32, (stations, stations), 0)
        load_bits().wait()
        load_codes().wait()
        for s in range(bits.shape[0]):
            word = jnp.zeros((stations, stations), jnp.int32)
            bit = column
            for w in range(bits.shape[1]):
                reached = column >= w * FLAG_BITS
                word = jnp.where(reached, bits[s, w], word)
                bit = jnp.where(reached, column - w * FLAG_BITS, bit)
            near = jnp.bitwise_and(jnp.right_shift(word, bit), 1).astype(jnp.float32).T
            if s == 0:
                chosen_ref[0] = near
            for code in codes_of(s):
                chosen_ref[place(s, code)] = near * jnp.where(codes[s] == code, 1.0, 0.0)

    def load_band(b, _):
        pl.when(b > 0)(load(b, False).start)
        load(b, True).start()
        return 0

    def send_other(b):
        whiten_rows(both, (0, b, OTHER), 0, stations)
        for q in range(PIECES):
            x_copy(b, q).start()

    def send_mine(b):
        whiten_rows(both, (0, b, keep_slot), 0, stations)
        pl.when(sends_z)(z_copy(b).start)

    def loaded(b):
        pltpu.make_async_copy(blk.at[b, pl.ds(0, 2)], blk.at[b, pl.ds(0, 2)], load_sem.at[b]).wait()

    for q in range(PIECES):
        load_first(q).start()
    barrier = pltpu.get_barrier_semaphore()
    peers = jnp.int32(0)
    for dr in (0, 1, -1):
        for col in (mate, c - 2, c + 2) if dr == 0 else (c, mate):
            there = (r + dr >= 0) & (r + dr < rows) & (col >= 0) & (col < cols)
            peers = peers + there.astype(jnp.int32)

            @pl.when(there)
            def _():
                pl.semaphore_signal(barrier, inc=1, device_id=(r + dr, col), device_id_type=MESH)
    lax.fori_loop(0, half, load_band, 0)
    for q in range(PIECES):
        load_first(q).wait()
        whiten_rows(both, (0, 0, OTHER), q * piece, piece)
        if q == 0:
            pl.semaphore_wait(barrier, peers)
        x_copy(0, q).start()
    load_codes().start()
    load_bits().start()
    load_old().start()
    load(0, True).wait()
    send_mine(0)
    loaded(1)
    send_mine(1)
    send_other(1)
    for step in range(AHEAD):
        for parity in (0, 1):
            pl.when(sides(parity))(side_copy(parity, jnp.int32(step)).start)

    def send_rest(b, _):
        loaded(b)
        send_other(b)
        send_mine(b)
        return 0

    lax.fori_loop(2, half, send_rest, 0)

    def own_product(b):
        for slot, band in ((keep_slot, half * odd + b), (OTHER, half * (1 - odd) + b)):
            view = View(both, (0, b, slot), segments)
            real, imag = product(view, view, scale)
            near = chosen_ref[0] > 0.5
            own_ref[band, 0] += jnp.where(near, real, 0.0)
            own_ref[band, 1] += jnp.where(near, imag, 0.0)

    def routes(b):
        is_odd = lax.rem(b, 2)
        even = is_odd == 0
        band, other_band = half * odd + b, half * (1 - odd) + b
        near = odd == 0
        left, mid, right = (0, b, 0), (0, b, 1), (0, b, 2)
        mid_above, mid_below = (1, b, 0), (1, b, 1)
        keeps = (is_odd, b, keep_slot + is_odd * (2 - keep_slot)), (1 - is_odd, b, 2 + is_odd * (keep_slot - 2))
        return [
            (0, left, mid, 3, band, r, first_col, left_pair, near),
            (1, mid, right, 3, band, r, mate, right_pair, None),
            (2, *keeps, 1, band, r - is_odd, c, meets(is_odd), even),
            (3, (is_odd, b, OTHER), (1 - is_odd, b, OTHER), 1, other_band, r - is_odd, c, meets(is_odd), even),
            (4, left, mid_below, 4, band, r, first_col, below & left_pair, near),
            (5, mid_above, right, 4, band, r - 1, mate, above & right_pair, None),
            (6, left, mid_above, 2, band, r, first_col, above & left_pair, near),
            (7, mid_below, right, 2, band, r + 1, mate, below & right_pair, None),
        ]

    def emit(b, route, go=True):
        which, left, right, code, band, row, col, present, local = route

        @pl.when(present)
        def _():
            real, imag = product(View(both, left, segments), View(both, right, segments), scale)
            real, imag = real.astype(jnp.bfloat16), imag.astype(jnp.bfloat16)

            def remote():
                stage[b, which, 0] = real
                stage[b, which, 1] = imag
                pl.when(go)(r_copy(b, which, code, band, row, col).start)

            if local is None:
                remote()
            else:
                @pl.when(local)
                def _():
                    c_ref[code - 1, band, 0] = real
                    c_ref[code - 1, band, 1] = imag

                pl.when(jnp.logical_not(local))(remote)

    last = jnp.where(lax.rem(r, 2) == 0, 1, jnp.where((r == 1) & (c == 1), 7, 5))

    def fire(a, held):
        table = routes(a)
        for which in ACROSS:
            _, _, _, code, band, row, col, present, _ = table[which]
            turn = (last == which) == held
            pl.when(present & turn)(r_copy(a, which, code, band, row, col).start)

    def step(b, _):
        for q in range(PIECES):
            @pl.when(b < half)
            def _():
                if q == 3:
                    @pl.when(b == half - 1)
                    def _():
                        for a in range(half - 1):
                            fire(a, False)
                        for a in range(EARLY):
                            fire(a, True)
                x_copy(b, q).wait_recv()
                for d, there in ((0, below), (1, above)):
                    pl.when(there)(mid_copy(b, q, d).start)
                at = b * PIECES + q + AHEAD
                for parity in (0, 1):
                    pl.when(sides(parity) & (at < 2 * PIECES * turns[parity]))(side_copy(parity, at).start)

            @pl.when(b == 0)
            def _():
                for a in range(q, half, PIECES):
                    own_product(a)

            @pl.when(b > 0)
            def _():
                a = b - 1
                table = routes(a)
                for which in ORDER[2 * q: 2 * q + 2]:
                    if which == 1:
                        pl.when(has_halo)(z_copy(a).wait_recv)
                    if which == 5:
                        pl.when(above)(whole(far.at[a, 0], ms.at[0], mr.at[a, 0]).wait_recv)
                    if which == 7:
                        pl.when(below)(whole(far.at[a, 1], ms.at[0], mr.at[a, 1]).wait_recv)
                    if which == 2:
                        pl.when(meets(lax.rem(a, 2)))(
                            whole(far.at[a, pl.ds(2, 2)], ms.at[0], kr.at[a]).wait_recv)
                    emit(a, table[which], (a == half - 1) & (last != which) if which in ACROSS else True)
                    if which == 7:
                        @pl.when(a == half - 1)
                        def _():
                            for e in range(EARLY, half):
                                fire(e, True)
        return 0

    unpack()
    load_old().wait()
    lax.fori_loop(0, half + 1, step, 0)

    whole(blk.at[:, OTHER], xs.at[0], xr.at[0, 0]).wait_send()
    pl.when(sends_z)(whole(blk.at[:, OTHER], zs.at[0], xr.at[0, 0]).wait_send)
    for d, there in ((0, below), (1, above)):
        pl.when(there)(whole(blk.at[:, pl.ds(0, 2)], ms.at[d], xr.at[0, 0]).wait_send)
    for group, there in enumerate((right_pair, above & right_pair, below & right_pair)):
        pl.when(there)(results(half, group).wait_send)
    for group, there in enumerate((left_pair, below & left_pair, above & left_pair), 3):
        pl.when(there & (odd == 1))(results(half, group).wait_send)
    pl.when(meets(1))(results(2 * turns[1], 6).wait_send)

    next_col = c + 1 < cols
    pl.when(below)(results(2 * turns[1], code=1).wait_recv)
    for code, comes in ((2, above & next_col), (3, next_col), (4, below & next_col)):
        pl.when(comes & (odd == 1))(results(2 * half, code=code).wait_recv)
        pl.when(comes & (odd == 0))(results(half, code=code).wait_recv)


def crosses(spectra, codes, range_bits, old, rows, cols):
    segments, parts, stations, bins = spectra.shape[2:]
    slots, bands, words = old.shape[2], old.shape[3], range_bits.shape[4]
    half, width = bands // 2, bins // bands
    hbm = pl.BlockSpec(memory_space=pltpu.MemorySpace.HBM)
    vmem = pl.BlockSpec(memory_space=pltpu.VMEM)
    bits = jnp.transpose(range_bits, (0, 2, 4, 1, 3))
    dma = pltpu.SemaphoreType.DMA
    return pl.pallas_call(
        functools.partial(cross_kernel, rows, cols),
        out_shape=(
            jax.ShapeDtypeStruct((bands, 2, stations, stations), jnp.float32),
            jax.ShapeDtypeStruct((place(slots, slots), stations, stations), jnp.float32),
            jax.ShapeDtypeStruct((4, bands, 2, stations, stations), jnp.bfloat16),
        ),
        in_specs=[hbm] * 4,
        out_specs=(vmem, vmem, vmem),
        scratch_shapes=[
            pltpu.VMEM((2, half, 4, segments, parts, stations, width), jnp.bfloat16),
            pltpu.VMEM((half, 8, 2, stations, stations), jnp.bfloat16),
            pltpu.VMEM((slots, words, 1, stations), jnp.int32),
            pltpu.SMEM(codes.shape, jnp.int32),
            dma((PIECES,)), dma((half,)),
            dma((1,)), dma((half, PIECES)),
            dma((1,)), dma((half,)),
            dma((2,)), dma((half, 2)),
            dma((half,)),
            dma((7,)), dma((4,)),
        ],
        compiler_params=pltpu.CompilerParams(collective_id=0, has_side_effects=True, vmem_limit_bytes=48 * 1024 * 1024),
        name="crosses",
    )(
        spectra,
        pltpu.with_memory_space_constraint(codes, pltpu.HBM),
        pltpu.with_memory_space_constraint(bits, pltpu.HBM),
        old,
    )


def combine_kernel(own_ref, chosen_ref, c_ref, old_ref, out_ref, done, own_sem, sem):
    slots, bands = old_ref.shape[2:4]
    own = pltpu.make_async_copy(own_ref, out_ref.at[0, 0, 0], own_sem)
    own.start()
    for s in reversed(range(1, slots)):
        def band(k, _):
            total = old_ref[0, 0, s, k]
            for code in codes_of(s):
                near = chosen_ref[place(s, code)] > 0.5
                total = total + jnp.where(near, c_ref[code - 1, k].astype(jnp.float32), 0.0)
            done[s - 1, k] = total
            return 0

        lax.fori_loop(0, bands, band, 0)
        pltpu.make_async_copy(done.at[s - 1], out_ref.at[0, 0, s], sem).start()
    own.wait()
    pltpu.make_async_copy(done, out_ref.at[0, 0, pl.ds(1, slots - 1)], sem).wait()


def combine(own, chosen, cross, old):
    slots, bands, parts, stations = old.shape[2:6]
    return pl.pallas_call(
        combine_kernel,
        out_shape=jax.ShapeDtypeStruct(old.shape, old.dtype),
        in_specs=[pl.BlockSpec(memory_space=pltpu.VMEM)] * 4,
        out_specs=pl.BlockSpec(memory_space=pltpu.MemorySpace.HBM),
        scratch_shapes=[
            pltpu.VMEM((slots - 1, bands, parts, stations, stations), jnp.float32),
            pltpu.SemaphoreType.DMA(()),
            pltpu.SemaphoreType.DMA(()),
        ],
        compiler_params=pltpu.CompilerParams(vmem_limit_bytes=16 * 1024 * 1024),
        name="combine",
    )(own, chosen, cross, old)


def solution(mesh):
    rows, cols = mesh.shape["gx"], mesh.shape["gy"]

    def body(spectra, partner_codes, range_bits, old_stacks):
        own, chosen, cross = crosses(spectra, partner_codes[0, 0], range_bits, old_stacks, rows, cols)
        return combine(own, chosen, cross, old_stacks)

    return jax.shard_map(
        body,
        mesh=mesh,
        in_specs=(
            P("gx", "gy", None, None, None, None),
            P("gx", "gy", None),
            P("gx", "gy", None, None, None),
            P("gx", "gy", None, None, None, None, None),
        ),
        out_specs=P("gx", "gy", None, None, None, None, None),
        check_vma=False,
    )
```

```python
import functools
import math

import jax
import jax.numpy as jnp
from jax import lax
from jax.experimental import pallas as pl
from jax.experimental.pallas import tpu as pltpu
from jax.sharding import PartitionSpec as P

EPSILON = 1e-06
MESH = pl.DeviceIdType.MESH
FLAG_BITS = 30


def whiten_rows(ref, index, first, count):
    segments, parts, _, width = ref.shape[len(index):]
    chunk = 16

    def rows(i, _):
        at = pl.ds(pl.multiple_of(first + i * chunk, chunk), chunk)
        pieces = [ref[(*index, s, p, at)].astype(jnp.float32)
                  for s in range(segments) for p in range(parts)]
        total = pieces[0] * pieces[0]
        for v in pieces[1:]:
            total = total + v * v
        power = jnp.sum(total, axis=1, keepdims=True) * (1.0 / (len(pieces) * width))
        scale = lax.rsqrt(power + EPSILON)
        for s in range(segments):
            for p in range(parts):
                ref[(*index, s, p, at)] = (pieces[s * parts + p] * scale).astype(jnp.bfloat16)
        return 0

    lax.fori_loop(0, count // chunk, rows, 0, unroll=2)


def product(left, right, scale):
    segments = left.count
    total = None
    for s in range(segments):
        part = lax.dot_general(
            left(s), right(s), (((1,), (1,)), ((), ())), preferred_element_type=jnp.float32
        )
        total = part if total is None else total + part
    n = total.shape[0] // 2
    real = total[:n, :n] + total[n:, n:]
    imag = total[n:, :n] - total[:n, n:]
    return real * scale, imag * scale


class View:
    def __init__(self, ref, index, count):
        self.ref, self.index, self.count = ref, index, count

    def __call__(self, s):
        v = self.ref[(*self.index, s)]
        return v.reshape(v.shape[0] * v.shape[1], v.shape[2])


OTHER = 3
PIECES = 4
EARLY = 1
AHEAD = 8
ACROSS = (1, 5, 7)
LAST = 7
ORDER = (1, 5, 7, 0, 4, 6, 2, 3)
GROUP = (3, 0, 6, 6, 4, 1, 5, 2)


def codes_of(slot):
    return range(slot, 5) if slot else ()


def place(slot, code):
    return 1 + sum(len(codes_of(s)) for s in range(slot)) + code - slot


def cross_kernel(rows, cols, x_ref, codes_ref, bits_ref, old_ref, own_ref, chosen_ref, c_ref, both, stage,
                 bits, codes, first_sem, load_sem, xs, xr, zs, zr, ms, mr, kr, rs, rr):
    blk, far = both.at[0], both.at[1]
    half, segments, stations, width = both.shape[1], both.shape[3], both.shape[5], both.shape[6]
    scale = 1.0 / math.sqrt(segments * width)
    piece = stations // PIECES
    turns = [(half + 1 - parity) // 2 for parity in (0, 1)]
    r = lax.axis_index("gx")
    c = lax.axis_index("gy")
    odd = lax.rem(c, 2)
    mate = c + 1 - 2 * odd
    keep_slot = 2 * odd
    halo_slot = 2 - 2 * odd
    z_to = c - 2 + 4 * odd
    z_from = c + 2 - 4 * odd
    sends_z = (z_to >= 0) & (z_to < cols)
    has_halo = (z_from >= 0) & (z_from < cols)
    first_col = c - 2 * odd
    above = r > 0
    below = r + 1 < rows
    left_pair = (odd == 0) | has_halo
    right_pair = (odd == 1) | has_halo

    def strip(q):
        return pl.ds(q * piece if isinstance(q, int) else pl.multiple_of(q * piece, piece), piece)

    def bins(b, mine):
        band = half * (odd if mine else 1 - odd) + b
        return pl.ds(pl.multiple_of(band * width, width), width)

    def load(b, mine):
        slot = keep_slot if mine else OTHER
        return pltpu.make_async_copy(
            x_ref.at[0, 0, :, :, :, bins(b, mine)], blk.at[b, slot], load_sem.at[b])

    def load_first(q):
        return pltpu.make_async_copy(
            x_ref.at[0, 0, :, :, strip(q), bins(0, False)], blk.at[0, OTHER, :, :, strip(q)],
            first_sem.at[q])

    def x_copy(b, q):
        return pltpu.make_async_remote_copy(
            src_ref=blk.at[b, OTHER, :, :, strip(q)], dst_ref=blk.at[b, 1, :, :, strip(q)],
            send_sem=xs.at[0], recv_sem=xr.at[b, q],
            device_id=(r, mate), device_id_type=MESH)

    def z_copy(b):
        return pltpu.make_async_remote_copy(
            src_ref=blk.at[b, keep_slot], dst_ref=blk.at[b, halo_slot],
            send_sem=zs.at[0], recv_sem=zr.at[b], device_id=(r, z_to), device_id_type=MESH)

    def mid_copy(b, q, d):
        return pltpu.make_async_remote_copy(
            src_ref=blk.at[b, 1, :, :, strip(q)], dst_ref=far.at[b, d, :, :, strip(q)],
            send_sem=ms.at[d], recv_sem=mr.at[b, d],
            device_id=(r + 1 - 2 * d, c), device_id_type=MESH)

    def side_to(parity):
        return r - 1 + 2 * parity

    def sides(parity):
        to = side_to(parity)
        return (to >= 0) & (to < rows)

    def meets(parity):
        other_row = r + 1 - 2 * parity
        return (other_row >= 0) & (other_row < rows)

    def side_copy(parity, step):
        b = 2 * (step // (2 * PIECES)) + parity
        e = lax.rem(step // PIECES, 2)
        q = lax.rem(step, PIECES)
        slot = keep_slot + e * (OTHER - keep_slot)
        return pltpu.make_async_remote_copy(
            src_ref=blk.at[b, slot, :, :, strip(q)], dst_ref=far.at[b, 2 + e, :, :, strip(q)],
            send_sem=ms.at[1 - parity], recv_sem=kr.at[b],
            device_id=(side_to(parity), c), device_id_type=MESH)

    def whole(slots, send, recv):
        return pltpu.make_async_remote_copy(
            src_ref=slots, dst_ref=slots, send_sem=send, recv_sem=recv,
            device_id=(r, mate), device_id_type=MESH)

    def r_copy(b, which, code, band, row, col):
        return pltpu.make_async_remote_copy(
            src_ref=stage.at[b, which], dst_ref=c_ref.at[code - 1, band],
            send_sem=rs.at[GROUP[which]], recv_sem=rr.at[code - 1],
            device_id=(row, col), device_id_type=MESH)

    def results(count, send=0, code=1):
        return whole(c_ref.at[0, pl.ds(0, count)], rs.at[send], rr.at[code - 1])

    def load_codes():
        return pltpu.make_async_copy(codes_ref, codes, first_sem.at[0])

    def load_bits():
        return pltpu.make_async_copy(bits_ref.at[0], bits, first_sem.at[1])

    def load_old():
        return pltpu.make_async_copy(old_ref.at[0, 0, 0], own_ref, first_sem.at[2])

    def unpack():
        column = lax.broadcasted_iota(jnp.int32, (stations, stations), 0)
        load_bits().wait()
        load_codes().wait()
        for s in range(bits.shape[0]):
            word = jnp.zeros((stations, stations), jnp.int32)
            bit = column
            for w in range(bits.shape[1]):
                reached = column >= w * FLAG_BITS
                word = jnp.where(reached, bits[s, w], word)
                bit = jnp.where(reached, column - w * FLAG_BITS, bit)
            near = jnp.bitwise_and(jnp.right_shift(word, bit), 1).astype(jnp.float32).T
            if s == 0:
                chosen_ref[0] = near
            for code in codes_of(s):
                chosen_ref[place(s, code)] = near * jnp.where(codes[s] == code, 1.0, 0.0)

    def load_band(b, _):
        pl.when(b > 0)(load(b, False).start)
        load(b, True).start()
        return 0

    def send_other(b):
        whiten_rows(both, (0, b, OTHER), 0, stations)
        for q in range(PIECES):
            x_copy(b, q).start()

    def send_mine(b):
        whiten_rows(both, (0, b, keep_slot), 0, stations)
        pl.when(sends_z)(z_copy(b).start)

    def loaded(b):
        pltpu.make_async_copy(blk.at[b, pl.ds(0, 2)], blk.at[b, pl.ds(0, 2)], load_sem.at[b]).wait()

    for q in range(PIECES):
        load_first(q).start()
    barrier = pltpu.get_barrier_semaphore()
    peers = jnp.int32(0)
    for dr in (0, 1, -1):
        for col in (mate, c - 2, c + 2) if dr == 0 else (c, mate):
            there = (r + dr >= 0) & (r + dr < rows) & (col >= 0) & (col < cols)
            peers = peers + there.astype(jnp.int32)

            @pl.when(there)
            def _():
                pl.semaphore_signal(barrier, inc=1, device_id=(r + dr, col), device_id_type=MESH)
    lax.fori_loop(0, half, load_band, 0)
    for q in range(PIECES):
        load_first(q).wait()
        whiten_rows(both, (0, 0, OTHER), q * piece, piece)
        if q == 0:
            pl.semaphore_wait(barrier, peers)
        x_copy(0, q).start()
    load_codes().start()
    load_bits().start()
    load_old().start()
    load(0, True).wait()
    send_mine(0)
    loaded(1)
    send_mine(1)
    send_other(1)
    for step in range(AHEAD):
        for parity in (0, 1):
            pl.when(sides(parity))(side_copy(parity, jnp.int32(step)).start)

    def send_rest(b, _):
        loaded(b)
        send_other(b)
        send_mine(b)
        return 0

    lax.fori_loop(2, half, send_rest, 0)

    def own_product(b):
        for slot, band in ((keep_slot, half * odd + b), (OTHER, half * (1 - odd) + b)):
            view = View(both, (0, b, slot), segments)
            real, imag = product(view, view, scale)
            near = chosen_ref[0] > 0.5
            own_ref[band, 0] += jnp.where(near, real, 0.0)
            own_ref[band, 1] += jnp.where(near, imag, 0.0)

    def routes(b):
        is_odd = lax.rem(b, 2)
        even = is_odd == 0
        band, other_band = half * odd + b, half * (1 - odd) + b
        near = odd == 0
        left, mid, right = (0, b, 0), (0, b, 1), (0, b, 2)
        mid_above, mid_below = (1, b, 0), (1, b, 1)
        keeps = (is_odd, b, keep_slot + is_odd * (2 - keep_slot)), (1 - is_odd, b, 2 + is_odd * (keep_slot - 2))
        return [
            (0, left, mid, 3, band, r, first_col, left_pair, near),
            (1, mid, right, 3, band, r, mate, right_pair, None),
            (2, *keeps, 1, band, r - is_odd, c, meets(is_odd), even),
            (3, (is_odd, b, OTHER), (1 - is_odd, b, OTHER), 1, other_band, r - is_odd, c, meets(is_odd), even),
            (4, left, mid_below, 4, band, r, first_col, below & left_pair, near),
            (5, mid_above, right, 4, band, r - 1, mate, above & right_pair, None),
            (6, left, mid_above, 2, band, r, first_col, above & left_pair, near),
            (7, mid_below, right, 2, band, r + 1, mate, below & right_pair, None),
        ]

    def emit(b, route, go=True):
        which, left, right, code, band, row, col, present, local = route

        @pl.when(present)
        def _():
            real, imag = product(View(both, left, segments), View(both, right, segments), scale)
            real, imag = real.astype(jnp.bfloat16), imag.astype(jnp.bfloat16)

            def remote():
                stage[b, which, 0] = real
                stage[b, which, 1] = imag
                pl.when(go)(r_copy(b, which, code, band, row, col).start)

            if local is None:
                remote()
            else:
                @pl.when(local)
                def _():
                    c_ref[code - 1, band, 0] = real
                    c_ref[code - 1, band, 1] = imag

                pl.when(jnp.logical_not(local))(remote)


    def fire(a, held):
        table = routes(a)
        for which in ACROSS:
            _, _, _, code, band, row, col, present, _ = table[which]
            turn = (which == LAST) == held
            if turn:
                pl.when(present)(r_copy(a, which, code, band, row, col).start)

    def step(b, _):
        for q in range(PIECES):
            @pl.when(b < half)
            def _():
                if q == 3:
                    @pl.when(b == half - 1)
                    def _():
                        for a in range(half - 1):
                            fire(a, False)
                        for a in range(EARLY):
                            fire(a, True)
                x_copy(b, q).wait_recv()
                for d, there in ((0, below), (1, above)):
                    pl.when(there)(mid_copy(b, q, d).start)
                at = b * PIECES + q + AHEAD
                for parity in (0, 1):
                    pl.when(sides(parity) & (at < 2 * PIECES * turns[parity]))(side_copy(parity, at).start)

            @pl.when(b == 0)
            def _():
                for a in range(q, half, PIECES):
                    own_product(a)

            @pl.when(b > 0)
            def _():
                a = b - 1
                table = routes(a)
                for which in ORDER[2 * q: 2 * q + 2]:
                    if which == 1:
                        pl.when(has_halo)(z_copy(a).wait_recv)
                    if which == 5:
                        pl.when(above)(whole(far.at[a, 0], ms.at[0], mr.at[a, 0]).wait_recv)
                    if which == 7:
                        pl.when(below)(whole(far.at[a, 1], ms.at[0], mr.at[a, 1]).wait_recv)
                    if which == 2:
                        pl.when(meets(lax.rem(a, 2)))(
                            whole(far.at[a, pl.ds(2, 2)], ms.at[0], kr.at[a]).wait_recv)
                    emit(a, table[which], (a == half - 1) & (which != LAST) if which in ACROSS else True)
                    if which == 7:
                        @pl.when(a == half - 1)
                        def _():
                            for e in range(EARLY, half):
                                fire(e, True)
        return 0

    unpack()
    load_old().wait()
    lax.fori_loop(0, half + 1, step, 0)

    whole(blk.at[:, OTHER], xs.at[0], xr.at[0, 0]).wait_send()
    pl.when(sends_z)(whole(blk.at[:, OTHER], zs.at[0], xr.at[0, 0]).wait_send)
    for d, there in ((0, below), (1, above)):
        pl.when(there)(whole(blk.at[:, pl.ds(0, 2)], ms.at[d], xr.at[0, 0]).wait_send)
    for group, there in enumerate((right_pair, above & right_pair, below & right_pair)):
        pl.when(there)(results(half, group).wait_send)
    for group, there in enumerate((left_pair, below & left_pair, above & left_pair), 3):
        pl.when(there & (odd == 1))(results(half, group).wait_send)
    pl.when(meets(1))(results(2 * turns[1], 6).wait_send)

    next_col = c + 1 < cols
    pl.when(below)(results(2 * turns[1], code=1).wait_recv)
    for code, comes in ((2, above & next_col), (3, next_col), (4, below & next_col)):
        pl.when(comes & (odd == 1))(results(2 * half, code=code).wait_recv)
        pl.when(comes & (odd == 0))(results(half, code=code).wait_recv)


def crosses(spectra, codes, range_bits, old, rows, cols):
    segments, parts, stations, bins = spectra.shape[2:]
    slots, bands, words = old.shape[2], old.shape[3], range_bits.shape[4]
    half, width = bands // 2, bins // bands
    hbm = pl.BlockSpec(memory_space=pltpu.MemorySpace.HBM)
    vmem = pl.BlockSpec(memory_space=pltpu.VMEM)
    bits = jnp.transpose(range_bits, (0, 2, 4, 1, 3))
    dma = pltpu.SemaphoreType.DMA
    return pl.pallas_call(
        functools.partial(cross_kernel, rows, cols),
        out_shape=(
            jax.ShapeDtypeStruct((bands, 2, stations, stations), jnp.float32),
            jax.ShapeDtypeStruct((place(slots, slots), stations, stations), jnp.float32),
            jax.ShapeDtypeStruct((4, bands, 2, stations, stations), jnp.bfloat16),
        ),
        in_specs=[hbm] * 4,
        out_specs=(vmem, vmem, vmem),
        scratch_shapes=[
            pltpu.VMEM((2, half, 4, segments, parts, stations, width), jnp.bfloat16),
            pltpu.VMEM((half, 8, 2, stations, stations), jnp.bfloat16),
            pltpu.VMEM((slots, words, 1, stations), jnp.int32),
            pltpu.SMEM(codes.shape, jnp.int32),
            dma((PIECES,)), dma((half,)),
            dma((1,)), dma((half, PIECES)),
            dma((1,)), dma((half,)),
            dma((2,)), dma((half, 2)),
            dma((half,)),
            dma((7,)), dma((4,)),
        ],
        compiler_params=pltpu.CompilerParams(collective_id=0, has_side_effects=True, vmem_limit_bytes=48 * 1024 * 1024),
        name="crosses",
    )(
        spectra,
        pltpu.with_memory_space_constraint(codes, pltpu.HBM),
        pltpu.with_memory_space_constraint(bits, pltpu.HBM),
        old,
    )


def combine_kernel(own_ref, chosen_ref, c_ref, old_ref, out_ref, done, own_sem, sem):
    slots, bands = old_ref.shape[2:4]
    own = pltpu.make_async_copy(own_ref, out_ref.at[0, 0, 0], own_sem)
    own.start()
    for s in reversed(range(1, slots)):
        def band(k, _):
            total = old_ref[0, 0, s, k]
            for code in codes_of(s):
                near = chosen_ref[place(s, code)] > 0.5
                total = total + jnp.where(near, c_ref[code - 1, k].astype(jnp.float32), 0.0)
            done[s - 1, k] = total
            return 0

        lax.fori_loop(0, bands, band, 0)
        pltpu.make_async_copy(done.at[s - 1], out_ref.at[0, 0, s], sem).start()
    own.wait()
    pltpu.make_async_copy(done, out_ref.at[0, 0, pl.ds(1, slots - 1)], sem).wait()


def combine(own, chosen, cross, old):
    slots, bands, parts, stations = old.shape[2:6]
    return pl.pallas_call(
        combine_kernel,
        out_shape=jax.ShapeDtypeStruct(old.shape, old.dtype),
        in_specs=[pl.BlockSpec(memory_space=pltpu.VMEM)] * 4,
        out_specs=pl.BlockSpec(memory_space=pltpu.MemorySpace.HBM),
        scratch_shapes=[
            pltpu.VMEM((slots - 1, bands, parts, stations, stations), jnp.float32),
            pltpu.SemaphoreType.DMA(()),
            pltpu.SemaphoreType.DMA(()),
        ],
        compiler_params=pltpu.CompilerParams(vmem_limit_bytes=16 * 1024 * 1024),
        name="combine",
    )(own, chosen, cross, old)


def solution(mesh):
    rows, cols = mesh.shape["gx"], mesh.shape["gy"]

    def body(spectra, partner_codes, range_bits, old_stacks):
        own, chosen, cross = crosses(spectra, partner_codes[0, 0], range_bits, old_stacks, rows, cols)
        return combine(own, chosen, cross, old_stacks)

    return jax.shard_map(
        body,
        mesh=mesh,
        in_specs=(
            P("gx", "gy", None, None, None, None),
            P("gx", "gy", None),
            P("gx", "gy", None, None, None),
            P("gx", "gy", None, None, None, None, None),
        ),
        out_specs=P("gx", "gy", None, None, None, None, None),
        check_vma=False,
    )
```
